32 devices in a mesh: row: 4 (over y, x), col: 8 (over z, core).
Axes of the slice: x: 2, y: 2, z: 4, core: 2. Of those that a mesh axis runs over, the one named last changes fastest.
Arguments:
- basis: bfloat16 [40, 131072], P(None, ('row', 'col'))
- expand: float32 [3, 8, 40], replicated, may hold values from -1 to 1
- tiles: bfloat16 [3, 3072, 128, 128], P(None, ('row', 'col')), may hold values from -0.3125 to 0.3125
- tile_rows: int32 [3072], P(('row', 'col')), may hold values from 0 to 255, as said below
- tile_cols: int32 [3072], P(('row', 'col')), may hold values from 0 to 127
Outputs:
- new_block: float32 [8, 131072], P(None, ('row', 'col'))
- coefficients: float32 [8, 40], replicated
- factor: float32 [8, 8], replicated
The draws below stay inside these ranges and needn't reach their ends.
Inputs may be any that keep to these rules, and one draw needn't show every extreme that they name: `tile_rows`: each device's 96 tiles come in 8 runs of 12; the row tiles of run k are 12 distinct values from k * 32 to (k + 1) * 32 - 1.
All inputs are finite; a program needn't handle non-finite values.
Results may differ from the reference program's by a relative error of at most 0.0054.
Values may be sent and summed in bfloat16 or wider, within the bound.
No kernel may reach another device: no remote copies, remote signals or barrier semaphores. Data moves between devices by JAX's collectives and lax.ppermute only.
A program may use at most 64 MiB of HBM per device.

```python
import math
import jax
import jax.numpy as jnp
from jax import lax

LOC = 4096
CAP = 12
TILE = 128
KD = 40
BS = 8
TPD = 96
NTOT = 131072
N_ROW = 4
N_COL = 8


def draw_basis(key, part):
    key_noise, key_common, key_lean = jax.random.split(key, 3)
    random_part = jax.random.normal(key_noise, (KD, NTOT), jnp.float32)
    common = jax.random.normal(key_common, (NTOT,), jnp.float32)
    leaning = jax.random.uniform(key_lean, (KD,), jnp.float32, -0.7, 0.7)
    return (random_part + leaning[:, None] * common[None, :]).astype(jnp.bfloat16)


def draw_tile_rows(key, part):
    region = LOC // TILE
    runs = N_ROW * N_COL * N_COL
    subkeys = jax.random.split(jax.random.fold_in(key, 7), runs)
    chosen = jax.vmap(lambda subkey: jax.random.permutation(subkey, region))(subkeys)[:, :CAP]
    offsets = jnp.arange(runs, dtype=jnp.int32) % N_COL * region
    return (chosen.astype(jnp.int32) + offsets[:, None]).reshape(runs * CAP).astype(jnp.int32)


def with_ends(array, stream_key, smallest, high):
    extent = array.shape
    place = [jax.random.randint(jax.random.fold_in(stream_key, axis), (), 0, extent[axis]) for axis in range(len(extent))]
    array = array.at[tuple(place)].set(smallest)
    longest = extent.index(max(extent))
    place[longest] = (place[longest] + 1) % extent[longest]
    return array.at[tuple(place)].set(high)


def block_scale(key, extent, shards, least, high):
    def one(dim, blocks):
        heights = jax.random.uniform(jax.random.fold_in(jax.random.fold_in(key, 6), dim), (blocks,), jnp.float32, least / len(shards), high / len(shards))
        return jnp.repeat(jnp.exp(heights), extent[dim] // blocks).reshape((-1,) + (1,) * (len(extent) - dim - 1))

    factor_of = one(*shards[0])
    for cut in shards[1:]:
        factor_of = factor_of * one(*cut)
    return factor_of


def noise(key, shape, scale, reach, pieces=(), kind=jnp.bfloat16):
    values = jax.random.normal(key, shape, jnp.float32) * scale
    if len(pieces) > 0:
        values = block_scale(key, shape, pieces, -0.22, 0.18) * values
    return jnp.clip(values, min=-reach, max=reach).astype(kind)


def setup_inputs(seed: int = 0) -> dict:
    key_of = jax.random.split(jax.random.key(seed), 6)
    return {
        "basis": draw_basis(jax.random.fold_in(key_of[5], 71), 0),
        "expand": noise(key_of[1], (3, BS, KD), KD ** -0.5, 1.0, (), jnp.float32),
        "tiles": noise(key_of[2], (3, TPD * N_ROW * N_COL, TILE, TILE), (TPD * TILE * TILE // LOC) ** -0.5, 0.3125, ((1, 32),)),
        "tile_rows": draw_tile_rows(jax.random.fold_in(key_of[5], 71), 0),
        "tile_cols": with_ends(jax.random.randint(key_of[4], (TPD * N_ROW * N_COL,), 0, N_ROW * LOC // TILE), jax.random.fold_in(key_of[4], 1), 0, (N_ROW * LOC // TILE) - 1).astype(jnp.int32),
    }


def reference(basis, expand, tiles, tile_rows, tile_cols):
    entries = LOC * N_ROW * N_COL
    inverse_root = 1.0 / math.sqrt(entries)
    highest = lax.Precision.HIGHEST
    basis_full = basis.astype(jnp.float32)
    series = jnp.einsum('mbk,kn->mbn', expand.astype(jnp.float32), basis_full, precision=highest).astype(jnp.bfloat16)
    layout = series.reshape(3, BS, N_ROW, N_COL, LOC)
    region = LOC // TILE
    slot_count = N_COL * region

    def device(index_dev, sums_row):
        index_dev = index_dev.astype(jnp.int32)
        row_index = index_dev // N_COL
        col_index = index_dev % N_COL
        columns = lax.dynamic_index_in_dim(layout, col_index, 3, keepdims=False)
        columns = columns.reshape(3, BS, N_ROW * LOC // TILE, TILE)
        start = (index_dev * TPD).astype(jnp.int32)
        matrices = lax.dynamic_slice_in_dim(tiles, start, TPD, 1).astype(jnp.float32)
        rows_here = lax.dynamic_slice_in_dim(tile_rows, start, TPD, 0)
        cols_here = lax.dynamic_slice_in_dim(tile_cols, start, TPD, 0)
        picked = jnp.take(columns, cols_here, axis=2).astype(jnp.float32)
        products = jnp.einsum('mtij,mbtj->bti', matrices, picked, precision=highest)
        onehot = (rows_here[:, None] == jnp.arange(slot_count, dtype=jnp.int32)[None, :]).astype(jnp.float32)
        partial_value = jnp.einsum('ts,bti->bsi', onehot, products, precision=highest).reshape(BS, slot_count * TILE)
        return sums_row.at[:, row_index].add(partial_value)
    sums_row = lax.fori_loop(0, N_ROW * N_COL, device, jnp.zeros((BS, N_ROW, slot_count * TILE), jnp.float32))
    applied = sums_row.reshape(BS, entries)
    first_pass = jnp.dot(applied, basis_full.T, precision=highest) * inverse_root
    projected = applied - jnp.dot(first_pass, basis_full, precision=highest) * inverse_root
    second_pass = jnp.dot(projected, basis_full.T, precision=highest) * inverse_root
    cleaned = projected - jnp.dot(second_pass, basis_full, precision=highest) * inverse_root
    coefficients = first_pass + second_pass
    gram_block = jnp.dot(cleaned, cleaned.T, precision=highest) / entries
    factor = jnp.linalg.cholesky(gram_block)
    new_block = lax.linalg.triangular_solve(factor, cleaned, left_side=True, lower=True)
    return (new_block, coefficients, factor)
```

```python
import functools
import math

import jax
import jax.numpy as jnp
from jax import lax
from jax.experimental import pallas as pl
from jax.experimental.pallas import tpu as pltpu
from jax.sharding import PartitionSpec as P

F32 = jnp.float32
BF16 = jnp.bfloat16
HALF = 64


def contract_lanes(a, b):
    return lax.dot_general(a, b, (((1,), (1,)), ((), ())), preferred_element_type=F32)


def split3(value):
    high = value.astype(BF16).astype(F32)
    rest = value - high
    middle = rest.astype(BF16).astype(F32)
    return high, middle, rest - middle


def series_kernel(region, tile, extra, basis_ref, expand_ref, out_ref, scratch):
    rows, krylov = expand_ref.shape
    basis = basis_ref[...]
    parts = jnp.concatenate(split3(expand_ref[...]), axis=0).astype(BF16)
    wide = jnp.dot(parts, basis, preferred_element_type=F32)
    series = (wide[:rows] + wide[rows : 2 * rows] + wide[2 * rows :]).astype(BF16)
    for t in range(region):
        out_ref[t] = series[:, t * tile : (t + 1) * tile]
    local = contract_lanes(basis, basis)
    high = local.astype(BF16).astype(F32)
    scratch[...] = jnp.zeros_like(scratch)
    scratch[:krylov, :krylov] = high
    scratch[:krylov, HALF : HALF + krylov] = local - high
    for e in range(extra):
        out_ref[region + e] = scratch[e * rows : (e + 1) * rows, :].astype(BF16)


def tile_kernel(
    sizes, cols_ref, rows_ref, gathered_ref, tiles_ref, mine_ref, other_ref, scratch, slices
):
    row_count, region, extra, krylov, cap, vectors, share = sizes
    col_count = slices.shape[0]
    tile = tiles_ref.shape[2]
    position = lax.axis_index("col")
    rows = gathered_ref.shape[2]

    total = jnp.zeros((extra * rows, tile), F32)
    for r in range(row_count):
        total += jnp.concatenate(
            [gathered_ref[r, region + e].astype(F32) for e in range(extra)], axis=0
        )
    scratch[...] = jnp.zeros_like(scratch)
    merged = total[:krylov, :krylov] + total[:krylov, HALF : HALF + krylov]
    high = merged.astype(BF16).astype(F32)
    scratch[:krylov, :krylov] = high
    scratch[:krylov, HALF : HALF + krylov] = merged - high
    slices[...] = jnp.zeros_like(slices)
    for c in range(col_count):
        if c * share < krylov:
            slices[c, :share, :] = scratch[c * share : (c + 1) * share, :]

    lane = lax.broadcasted_iota(jnp.int32, (8, tile), 1)
    sublane = lax.broadcasted_iota(jnp.int32, (8, tile), 0)
    slot = lane // vectors
    inner = lane - slot * vectors

    def column(t):
        c = cols_ref[t]
        r = c // region
        return gathered_ref[r, c - r * region]

    def block(relative, out_ref, half):
        target = (position ^ (2 * relative)) ^ half
        base = target * cap
        for p in range(cap // 2):
            t0 = base + 2 * p
            x0 = column(t0)
            x1 = column(t0 + 1)
            out = None
            for m in range(3):
                lhs = jnp.concatenate(
                    [x0[m * vectors : (m + 1) * vectors], x1[m * vectors : (m + 1) * vectors]],
                    axis=0,
                )
                rhs = tiles_ref[m, pl.ds(t0, 2)].reshape(2 * tile, tile)
                term = contract_lanes(lhs, rhs)
                out = term if out is None else out + term
            pair = jnp.concatenate([out[:vectors, :tile], out[vectors:, tile:]], axis=0)
            out_ref[relative, 2 * p * vectors : (2 * p + 2) * vectors, :] = pair.astype(BF16)
        code = jnp.full((8, tile), -1, jnp.int32)
        for s in range(cap):
            code = jnp.where(
                slot == s, (rows_ref[base + s] - target * region) * vectors + inner, code
            )
        last = jnp.where(sublane == 7, code.astype(F32), slices[target])
        out_ref[relative, cap * vectors : (cap + 1) * vectors, :] = last.astype(BF16)

    for half, out_ref in ((1, other_ref), (0, mine_ref)):

        def step(relative, carry, half=half, out_ref=out_ref):
            block(relative, out_ref, half)
            return carry

        lax.fori_loop(0, col_count // 2, step, 0)


def merge_kernel(sizes, basis_ref, *refs):
    region, krylov, cap, vectors, share = sizes
    blocks, (applied_ref, packet_ref) = refs[:-2], refs[-2:]
    tile = applied_ref.shape[1] // region
    total = jnp.zeros((region * vectors, tile), F32)
    small = jnp.zeros((vectors, tile), F32)
    place = lax.broadcasted_iota(jnp.int32, (region * vectors, tile), 0).astype(F32)
    span = (cap + 1) * vectors
    for ref in blocks:
        for part in range(ref.shape[0]):
            piece = ref[part]
            last = piece[cap * vectors :].astype(F32)
            small += last
            onehot = jnp.where(place == last[7:8, :], 1.0, 0.0).astype(BF16)
            total += jnp.dot(onehot[:, :span], piece, preferred_element_type=F32)
    for t in range(region):
        applied_ref[:, t * tile : (t + 1) * tile] = total[t * vectors : (t + 1) * vectors]
    applied = applied_ref[...]
    high, middle, low = split3(applied)
    lhs = jnp.concatenate([high, middle], axis=0).astype(BF16)
    inner = contract_lanes(lhs, basis_ref[...])
    raw = inner[:vectors] + inner[vectors:]
    cross = contract_lanes(lhs, lhs)
    energy = (cross[:vectors, :vectors] + cross[vectors:, vectors:]) + (
        cross[:vectors, vectors:] + cross[vectors:, :vectors]
    )
    slice_rows = small[:, :krylov] + small[:, HALF : HALF + krylov]
    packet = jnp.concatenate(
        [
            raw,
            energy,
            jnp.zeros((vectors, HALF - krylov - vectors), F32),
            slice_rows,
            jnp.zeros((vectors, tile - HALF - krylov), F32),
        ],
        axis=1,
    )
    packet_ref[...] = jnp.broadcast_to(packet[None], packet_ref.shape)


def finish_kernel(
    sizes, packets_ref, applied_ref, basis_ref, new_ref, coefficients_ref, factor_ref, scratch
):
    krylov, vectors, share, col_count, entries = sizes
    inverse_root = 1.0 / math.sqrt(entries)
    highest = lax.Precision.HIGHEST
    total = packets_ref[0]
    for d in range(1, packets_ref.shape[0]):
        total += packets_ref[d]
    for c in range(col_count):
        count = min(share, krylov - c * share)
        if count > 0:
            scratch[c * share : c * share + count, :] = packets_ref[c, :count, :]
    correlation = scratch[:krylov, HALF : HALF + krylov] * (1.0 / entries)
    first = total[:, :krylov] * inverse_root
    energy = total[:, krylov : krylov + vectors]
    dot = functools.partial(jnp.dot, precision=highest, preferred_element_type=F32)
    across = functools.partial(
        lax.dot_general,
        dimension_numbers=(((1,), (1,)), ((), ())),
        precision=highest,
        preferred_element_type=F32,
    )
    coefficients = first + (first - dot(first, correlation))
    coefficients_ref[...] = coefficients
    parts = jnp.concatenate(split3(coefficients * inverse_root), axis=0).astype(BF16)
    wide = jnp.dot(parts, basis_ref[...], preferred_element_type=F32)
    cleaned = applied_ref[...] - (
        wide[:vectors] + (wide[vectors : 2 * vectors] + wide[2 * vectors :])
    )
    mixed = across(first, coefficients)
    mixed_t = across(coefficients, first)
    curved = across(dot(coefficients, correlation), coefficients)
    gram = (energy - mixed - mixed_t + curved) * (1.0 / entries)
    tile = packets_ref.shape[2]
    columns = [jnp.broadcast_to(gram[:, j : j + 1], (vectors, tile)) for j in range(vectors)]
    sublane = lax.broadcasted_iota(jnp.int32, (vectors, tile), 0)
    lane = lax.broadcasted_iota(jnp.int32, (vectors, tile), 1)
    factor = jnp.zeros((vectors, tile), F32)
    length = cleaned.shape[1]
    for j in range(vectors):
        inverse = lax.rsqrt(columns[j][j : j + 1, :])
        column = jnp.where(sublane >= j, columns[j] * inverse, 0.0)
        factor = jnp.where(lane == j, column, factor)
        for k in range(j + 1, vectors):
            columns[k] = columns[k] - column * column[k : k + 1, :]
        below = jnp.where(sublane > j, column, 0.0)
        pieces = []
        for t in range(length // tile):
            piece = cleaned[:, t * tile : (t + 1) * tile]
            row = piece[j : j + 1, :] * inverse
            pieces.append(jnp.where(sublane == j, row, piece - below * row))
        cleaned = jnp.concatenate(pieces, axis=1)
    factor_ref[...] = factor[:, :vectors]
    new_ref[...] = cleaned


def shards(basis, expand, tiles, tile_rows, tile_cols):
    row_count = lax.axis_size("row")
    col_count = lax.axis_size("col")
    krylov, length = basis.shape
    tile = tiles.shape[2]
    vectors = expand.shape[1]
    rows = expand.shape[0] * vectors
    region = length // tile
    devices = row_count * col_count
    entries = length * devices
    cap = tiles.shape[1] // col_count
    extra = -(-krylov // rows)
    share = -(-krylov // col_count)
    span = (cap + 1) * vectors
    assert krylov + vectors <= HALF and share < 8 and region * vectors <= 256
    vmem = pl.BlockSpec(memory_space=pltpu.VMEM)
    smem = pl.BlockSpec(memory_space=pltpu.SMEM)

    series = pl.pallas_call(
        functools.partial(series_kernel, region, tile, extra),
        out_shape=jax.ShapeDtypeStruct((region + extra, rows, tile), BF16),
        in_specs=[vmem, vmem],
        out_specs=vmem,
        scratch_shapes=[pltpu.VMEM((extra * rows, tile), F32)],
        name="series",
    )(basis, expand.reshape(rows, krylov))
    gathered = lax.all_gather(series, "row", axis=0)
    half = col_count // 2
    outgoing = jax.ShapeDtypeStruct((half, span, tile), BF16)
    mine, other = pl.pallas_call(
        functools.partial(
            tile_kernel, (row_count, region, extra, krylov, cap, vectors, share)
        ),
        out_shape=(outgoing, outgoing),
        in_specs=[smem, smem, vmem, vmem],
        out_specs=(vmem, vmem),
        scratch_shapes=[
            pltpu.VMEM((max(extra * rows, share * col_count), tile), F32),
            pltpu.VMEM((col_count, 8, tile), F32),
        ],
        name="products",
    )(tile_cols, tile_rows, gathered, tiles)
    partner = lax.ppermute(other, "col", [(i, i ^ 1) for i in range(col_count)])
    blocks = [mine[:1], partner[:1]]
    for relative in range(half - 1, 0, -1):
        pair = jnp.stack([mine[relative], partner[relative]])
        blocks.append(
            lax.ppermute(pair, "col", [(i, i ^ (2 * relative)) for i in range(col_count)])
        )
    applied, packet = pl.pallas_call(
        functools.partial(merge_kernel, (region, krylov, cap, vectors, share)),
        out_shape=(
            jax.ShapeDtypeStruct((vectors, length), F32),
            jax.ShapeDtypeStruct((devices, vectors, tile), F32),
        ),
        in_specs=[vmem] * (1 + len(blocks)),
        out_specs=(vmem, vmem),
        name="merge",
    )(basis, *blocks)
    packets = lax.all_to_all(packet, ("row", "col"), 0, 0, tiled=True)
    return pl.pallas_call(
        functools.partial(finish_kernel, (krylov, vectors, share, col_count, entries)),
        out_shape=(
            jax.ShapeDtypeStruct((vectors, length), F32),
            jax.ShapeDtypeStruct((vectors, krylov), F32),
            jax.ShapeDtypeStruct((vectors, vectors), F32),
        ),
        in_specs=[vmem] * 3,
        out_specs=(vmem,) * 3,
        scratch_shapes=[pltpu.VMEM((share * col_count, tile), F32)],
        name="finish",
    )(packets, applied, basis)


def solution(mesh):
    return jax.shard_map(
        shards,
        mesh=mesh,
        in_specs=(
            P(None, ("row", "col")),
            P(),
            P(None, ("row", "col"), None, None),
            P(("row", "col")),
            P(("row", "col")),
        ),
        out_specs=(P(None, ("row", "col")), P(), P()),
        check_vma=False,
    )
```

```python
import functools
import math

import jax
import jax.numpy as jnp
from jax import lax
from jax.experimental import pallas as pl
from jax.experimental.pallas import tpu as pltpu
from jax.sharding import PartitionSpec as P

F32 = jnp.float32
BF16 = jnp.bfloat16
HALF = 64


def contract_lanes(a, b):
    return lax.dot_general(a, b, (((1,), (1,)), ((), ())), preferred_element_type=F32)


def split3(value):
    high = value.astype(BF16).astype(F32)
    rest = value - high
    middle = rest.astype(BF16).astype(F32)
    return high, middle, rest - middle


def series_kernel(region, tile, extra, basis_ref, expand_ref, out_ref, scratch):
    rows, krylov = expand_ref.shape
    basis = basis_ref[...]
    parts = jnp.concatenate(split3(expand_ref[...]), axis=0).astype(BF16)
    wide = jnp.dot(parts, basis, preferred_element_type=F32)
    series = (wide[:rows] + wide[rows : 2 * rows] + wide[2 * rows :]).astype(BF16)
    for t in range(region):
        out_ref[t] = series[:, t * tile : (t + 1) * tile]
    local = contract_lanes(basis, basis)
    high = local.astype(BF16).astype(F32)
    scratch[...] = jnp.zeros_like(scratch)
    scratch[:krylov, :krylov] = high
    scratch[:krylov, HALF : HALF + krylov] = local - high
    for e in range(extra):
        out_ref[region + e] = scratch[e * rows : (e + 1) * rows, :].astype(BF16)


def tile_kernel(
    sizes, cols_ref, rows_ref, gathered_ref, tiles_ref, mine_ref, other_ref, scratch, slices
):
    row_count, region, extra, krylov, cap, vectors, share = sizes
    col_count = slices.shape[0]
    tile = tiles_ref.shape[2]
    position = lax.axis_index("col")
    rows = gathered_ref.shape[2]

    total = jnp.zeros((extra * rows, tile), F32)
    for r in range(row_count):
        total += jnp.concatenate(
            [gathered_ref[r, region + e].astype(F32) for e in range(extra)], axis=0
        )
    scratch[...] = jnp.zeros_like(scratch)
    merged = total[:krylov, :krylov] + total[:krylov, HALF : HALF + krylov]
    high = merged.astype(BF16).astype(F32)
    scratch[:krylov, :krylov] = high
    scratch[:krylov, HALF : HALF + krylov] = merged - high
    slices[...] = jnp.zeros_like(slices)
    for c in range(col_count):
        if c * share < krylov:
            slices[c, :share, :] = scratch[c * share : (c + 1) * share, :]

    lane = lax.broadcasted_iota(jnp.int32, (8, tile), 1)
    sublane = lax.broadcasted_iota(jnp.int32, (8, tile), 0)
    slot = lane // vectors
    inner = lane - slot * vectors

    def column(t):
        c = cols_ref[t]
        r = c // region
        return gathered_ref[r, c - r * region]

    def block(relative, out_ref, half):
        target = (position ^ (2 * relative)) ^ half
        base = target * cap
        for p in range(cap // 2):
            t0 = base + 2 * p
            x0 = column(t0)
            x1 = column(t0 + 1)
            out = None
            for m in range(3):
                lhs = jnp.concatenate(
                    [x0[m * vectors : (m + 1) * vectors], x1[m * vectors : (m + 1) * vectors]],
                    axis=0,
                )
                rhs = tiles_ref[m, pl.ds(t0, 2)].reshape(2 * tile, tile)
                term = contract_lanes(lhs, rhs)
                out = term if out is None else out + term
            pair = jnp.concatenate([out[:vectors, :tile], out[vectors:, tile:]], axis=0)
            out_ref[relative, 2 * p * vectors : (2 * p + 2) * vectors, :] = pair.astype(BF16)
        code = jnp.full((8, tile), -1, jnp.int32)
        for s in range(cap):
            code = jnp.where(
                slot == s, (rows_ref[base + s] - target * region) * vectors + inner, code
            )
        last = jnp.where(sublane == 7, code.astype(F32), slices[target])
        out_ref[relative, cap * vectors : (cap + 1) * vectors, :] = last.astype(BF16)

    for half, out_ref in ((1, other_ref), (0, mine_ref)):

        def step(relative, carry, half=half, out_ref=out_ref):
            block(relative, out_ref, half)
            return carry

        lax.fori_loop(0, col_count // 2, step, 0)


def merge_kernel(sizes, basis_ref, *refs):
    region, krylov, cap, vectors, share = sizes
    blocks, (applied_ref, packet_ref) = refs[:-2], refs[-2:]
    tile = applied_ref.shape[1] // region
    total = jnp.zeros((region * vectors, tile), F32)
    small = jnp.zeros((vectors, tile), F32)
    place = lax.broadcasted_iota(jnp.int32, (region * vectors, tile), 0).astype(F32)
    span = (cap + 1) * vectors
    for ref in blocks:
        for part in range(ref.shape[0]):
            piece = ref[part]
            last = piece[cap * vectors :].astype(F32)
            small += last
            onehot = jnp.where(place == last[7:8, :], 1.0, 0.0).astype(BF16)
            total += jnp.dot(onehot[:, :span], piece, preferred_element_type=F32)
    for t in range(region):
        applied_ref[:, t * tile : (t + 1) * tile] = total[t * vectors : (t + 1) * vectors]
    applied = applied_ref[...]
    high, middle, low = split3(applied)
    lhs = jnp.concatenate([high, middle], axis=0).astype(BF16)
    inner = contract_lanes(lhs, basis_ref[...])
    raw = inner[:vectors] + inner[vectors:]
    cross = contract_lanes(lhs, lhs)
    energy = (cross[:vectors, :vectors] + cross[vectors:, vectors:]) + (
        cross[:vectors, vectors:] + cross[vectors:, :vectors]
    )
    slice_rows = small[:, :krylov] + small[:, HALF : HALF + krylov]
    packet = jnp.concatenate(
        [
            raw,
            energy,
            jnp.zeros((vectors, HALF - krylov - vectors), F32),
            slice_rows,
            jnp.zeros((vectors, tile - HALF - krylov), F32),
        ],
        axis=1,
    )
    packet_ref[...] = jnp.broadcast_to(packet[None], packet_ref.shape)


def finish_kernel(
    sizes, packets_ref, applied_ref, basis_ref, new_ref, coefficients_ref, factor_ref, scratch
):
    krylov, vectors, share, col_count, entries = sizes
    inverse_root = 1.0 / math.sqrt(entries)
    highest = lax.Precision.HIGHEST
    total = packets_ref[0]
    for d in range(1, packets_ref.shape[0]):
        total += packets_ref[d]
    for c in range(col_count):
        count = min(share, krylov - c * share)
        if count > 0:
            scratch[c * share : c * share + count, :] = packets_ref[c, :count, :]
    correlation = scratch[:krylov, HALF : HALF + krylov] * (1.0 / entries)
    first = total[:, :krylov] * inverse_root
    energy = total[:, krylov : krylov + vectors]
    dot = functools.partial(jnp.dot, precision=highest, preferred_element_type=F32)
    across = functools.partial(
        lax.dot_general,
        dimension_numbers=(((1,), (1,)), ((), ())),
        precision=highest,
        preferred_element_type=F32,
    )
    coefficients = first + (first - dot(first, correlation))
    coefficients_ref[...] = coefficients
    parts = jnp.concatenate(split3(coefficients * inverse_root), axis=0).astype(BF16)
    wide = jnp.dot(parts, basis_ref[...], preferred_element_type=F32)
    cleaned = applied_ref[...] - (
        wide[:vectors] + (wide[vectors : 2 * vectors] + wide[2 * vectors :])
    )
    mixed = across(first, coefficients)
    mixed_t = across(coefficients, first)
    curved = across(dot(coefficients, correlation), coefficients)
    gram = (energy - mixed - mixed_t + curved) * (1.0 / entries)
    tile = packets_ref.shape[2]
    columns = [jnp.broadcast_to(gram[:, j : j + 1], (vectors, tile)) for j in range(vectors)]
    sublane = lax.broadcasted_iota(jnp.int32, (vectors, tile), 0)
    lane = lax.broadcasted_iota(jnp.int32, (vectors, tile), 1)
    factor = jnp.zeros((vectors, tile), F32)
    length = cleaned.shape[1]
    for j in range(vectors):
        inverse = lax.rsqrt(columns[j][j : j + 1, :])
        column = jnp.where(sublane >= j, columns[j] * inverse, 0.0)
        factor = jnp.where(lane == j, column, factor)
        for k in range(j + 1, vectors):
            columns[k] = columns[k] - column * column[k : k + 1, :]
        below = jnp.where(sublane > j, column, 0.0)
        pieces = []
        for t in range(length // tile):
            piece = cleaned[:, t * tile : (t + 1) * tile]
            row = piece[j : j + 1, :] * inverse
            pieces.append(jnp.where(sublane == j, row, piece - below * row))
        cleaned = jnp.concatenate(pieces, axis=1)
    factor_ref[...] = factor[:, :vectors]
    new_ref[...] = cleaned


def shards(basis, expand, tiles, tile_rows, tile_cols):
    row_count = lax.axis_size("row")
    col_count = lax.axis_size("col")
    krylov, length = basis.shape
    tile = tiles.shape[2]
    vectors = expand.shape[1]
    rows = expand.shape[0] * vectors
    region = length // tile
    devices = row_count * col_count
    entries = length * devices
    cap = tiles.shape[1] // col_count
    extra = -(-krylov // rows)
    share = -(-krylov // col_count)
    span = (cap + 1) * vectors
    assert krylov + vectors <= HALF and share < 8 and region * vectors <= 256
    vmem = pl.BlockSpec(memory_space=pltpu.VMEM)
    smem = pl.BlockSpec(memory_space=pltpu.SMEM)

    series = pl.pallas_call(
        functools.partial(series_kernel, region, tile, extra),
        out_shape=jax.ShapeDtypeStruct((region + extra, rows, tile), BF16),
        in_specs=[vmem, vmem],
        out_specs=vmem,
        scratch_shapes=[pltpu.VMEM((extra * rows, tile), F32)],
        compiler_params=pltpu.CompilerParams(vmem_limit_bytes=4 << 20),
        name="series",
    )(basis, expand.reshape(rows, krylov))
    gathered = lax.all_gather(series, "row", axis=0)
    half = col_count // 2
    outgoing = jax.ShapeDtypeStruct((half, span, tile), BF16)
    mine, other = pl.pallas_call(
        functools.partial(
            tile_kernel, (row_count, region, extra, krylov, cap, vectors, share)
        ),
        out_shape=(outgoing, outgoing),
        in_specs=[smem, smem, vmem, vmem],
        out_specs=(vmem, vmem),
        scratch_shapes=[
            pltpu.VMEM((max(extra * rows, share * col_count), tile), F32),
            pltpu.VMEM((col_count, 8, tile), F32),
        ],
        compiler_params=pltpu.CompilerParams(vmem_limit_bytes=16 << 20),
        name="products",
    )(tile_cols, tile_rows, gathered, tiles)
    partner = lax.ppermute(other, "col", [(i, i ^ 1) for i in range(col_count)])
    blocks = [mine[:1], partner[:1]]
    for relative in range(half - 1, 0, -1):
        pair = jnp.stack([mine[relative], partner[relative]])
        blocks.append(
            lax.ppermute(pair, "col", [(i, i ^ (2 * relative)) for i in range(col_count)])
        )
    applied, packet = pl.pallas_call(
        functools.partial(merge_kernel, (region, krylov, cap, vectors, share)),
        out_shape=(
            jax.ShapeDtypeStruct((vectors, length), F32),
            jax.ShapeDtypeStruct((devices, vectors, tile), F32),
        ),
        in_specs=[vmem] * (1 + len(blocks)),
        out_specs=(vmem, vmem),
        compiler_params=pltpu.CompilerParams(vmem_limit_bytes=8 << 20),
        name="merge",
    )(basis, *blocks)
    packets = lax.all_to_all(packet, ("row", "col"), 0, 0, tiled=True)
    return pl.pallas_call(
        functools.partial(finish_kernel, (krylov, vectors, share, col_count, entries)),
        out_shape=(
            jax.ShapeDtypeStruct((vectors, length), F32),
            jax.ShapeDtypeStruct((vectors, krylov), F32),
            jax.ShapeDtypeStruct((vectors, vectors), F32),
        ),
        in_specs=[vmem] * 3,
        out_specs=(vmem,) * 3,
        scratch_shapes=[pltpu.VMEM((share * col_count, tile), F32)],
        compiler_params=pltpu.CompilerParams(vmem_limit_bytes=4 << 20),
        name="finish",
    )(packets, applied, basis)


def solution(mesh):
    return jax.shard_map(
        shards,
        mesh=mesh,
        in_specs=(
            P(None, ("row", "col")),
            P(),
            P(None, ("row", "col"), None, None),
            P(("row", "col")),
            P(("row", "col")),
        ),
        out_specs=(P(None, ("row", "col")), P(), P()),
        check_vma=False,
    )
```

```python
import functools
import math

import jax
import jax.numpy as jnp
from jax import lax
from jax.experimental import pallas as pl
from jax.experimental.pallas import tpu as pltpu
from jax.sharding import PartitionSpec as P

F32 = jnp.float32
BF16 = jnp.bfloat16
HALF = 64


def contract_lanes(a, b):
    return lax.dot_general(a, b, (((1,), (1,)), ((), ())), preferred_element_type=F32)


def split3(value):
    high = value.astype(BF16).astype(F32)
    rest = value - high
    middle = rest.astype(BF16).astype(F32)
    return high, middle, rest - middle


def series_kernel(region, tile, extra, basis_ref, expand_ref, out_ref, scratch, here, small, sems):
    rows, krylov = expand_ref.shape
    copies = [
        pltpu.make_async_copy(basis_ref, here, sems.at[0]),
        pltpu.make_async_copy(expand_ref, small, sems.at[1]),
    ]
    for copy in copies:
        copy.start()
    scratch[...] = jnp.zeros_like(scratch)
    for copy in copies:
        copy.wait()
    basis = here[...]
    parts = jnp.concatenate(split3(small[...]), axis=0).astype(BF16)
    wide = jnp.dot(parts, basis, preferred_element_type=F32)
    series = (wide[:rows] + wide[rows : 2 * rows] + wide[2 * rows :]).astype(BF16)
    for t in range(region):
        out_ref[t] = series[:, t * tile : (t + 1) * tile]
    local = contract_lanes(basis, basis)
    high = local.astype(BF16).astype(F32)
    scratch[:krylov, :krylov] = high
    scratch[:krylov, HALF : HALF + krylov] = local - high
    for e in range(extra):
        out_ref[region + e] = scratch[e * rows : (e + 1) * rows, :].astype(BF16)


def tile_kernel(
    sizes, cols_ref, rows_ref, gathered_ref, tiles_ref, mine_ref, other_ref, scratch, slices
):
    row_count, region, extra, krylov, cap, vectors, share = sizes
    col_count = slices.shape[0]
    tile = tiles_ref.shape[2]
    position = lax.axis_index("col")
    rows = gathered_ref.shape[2]

    total = jnp.zeros((extra * rows, tile), F32)
    for r in range(row_count):
        total += jnp.concatenate(
            [gathered_ref[r, region + e].astype(F32) for e in range(extra)], axis=0
        )
    scratch[...] = jnp.zeros_like(scratch)
    merged = total[:krylov, :krylov] + total[:krylov, HALF : HALF + krylov]
    high = merged.astype(BF16).astype(F32)
    scratch[:krylov, :krylov] = high
    scratch[:krylov, HALF : HALF + krylov] = merged - high
    slices[...] = jnp.zeros_like(slices)
    for c in range(col_count):
        if c * share < krylov:
            slices[c, :share, :] = scratch[c * share : (c + 1) * share, :]

    lane = lax.broadcasted_iota(jnp.int32, (8, tile), 1)
    sublane = lax.broadcasted_iota(jnp.int32, (8, tile), 0)
    slot = lane // vectors
    inner = lane - slot * vectors

    def column(t):
        c = cols_ref[t]
        r = lax.div(c, region)
        x = gathered_ref[r, c - r * region]
        return [x[m * vectors : (m + 1) * vectors] for m in range(3)]

    def weights(m, t):
        return tiles_ref[m, pl.ds(t, 2)].reshape(2 * tile, tile)

    def side(a, b):
        return jnp.concatenate([a, b], axis=1)

    def block(relative, half, out_ref):
        target = (position ^ (2 * relative)) ^ half
        base = target * cap

        def store(p, out):
            pair = jnp.concatenate([out[:vectors, :tile], out[vectors:, tile:]], axis=0)
            out_ref[relative, 2 * p * vectors : (2 * p + 2) * vectors, :] = pair.astype(BF16)

        pairs = []
        for p in range(cap // 2):
            t = base + 2 * p
            x0, x1 = column(t), column(t + 1)
            lhs = jnp.concatenate([side(x0[0], x0[1]), side(x1[0], x1[1])], axis=0)
            rhs = side(weights(0, t), weights(1, t))
            third = jnp.concatenate([x0[2], x1[2]], axis=0)
            pairs.append((p, contract_lanes(lhs, rhs), third, weights(2, t)))
        while len(pairs) > 1:
            (p, out_p, x_p, w_p), (q, out_q, x_q, w_q) = pairs[:2]
            pairs = pairs[2:]
            zero = jnp.zeros_like(x_p)
            lhs = jnp.concatenate([side(x_p, zero), side(zero, x_q)], axis=0)
            both = contract_lanes(lhs, side(w_p, w_q))
            store(p, out_p + both[: 2 * vectors])
            store(q, out_q + both[2 * vectors :])
        for p, out_p, x_p, w_p in pairs:
            store(p, out_p + contract_lanes(x_p, w_p))
        code = jnp.full((8, tile), -1, jnp.int32)
        for s in range(cap):
            code = jnp.where(
                slot == s, (rows_ref[base + s] - target * region) * vectors + inner, code
            )
        last = jnp.where(sublane == 7, code.astype(F32), slices[target])
        out_ref[relative, cap * vectors : (cap + 1) * vectors, :] = last.astype(BF16)

    for half, out_ref in ((1, other_ref), (0, mine_ref)):
        for relative in range(col_count // 2):
            block(relative, half, out_ref)


def merge_kernel(sizes, basis_ref, *refs):
    region, krylov, cap, vectors, each = sizes
    blocks, (applied_ref, packet_ref, scratch) = refs[:-3], refs[-3:]
    tile = applied_ref.shape[1] // region
    total = jnp.zeros((region * vectors, tile), F32)
    small = jnp.zeros((vectors, tile), F32)
    place = lax.broadcasted_iota(jnp.int32, (region * vectors, tile), 0).astype(F32)
    span = (cap + 1) * vectors
    for ref in blocks:
        for part in range(ref.shape[0]):
            piece = ref[part]
            last = piece[cap * vectors :].astype(F32)
            small += last
            onehot = jnp.where(place == last[7:8, :], 1.0, 0.0).astype(BF16)
            total += jnp.dot(onehot[:, :span], piece, preferred_element_type=F32)
    for t in range(region):
        applied_ref[:, t * tile : (t + 1) * tile] = total[t * vectors : (t + 1) * vectors]
    applied = applied_ref[...]
    high, middle, low = split3(applied)
    lhs = jnp.concatenate([high, middle], axis=0).astype(BF16)
    inner = contract_lanes(lhs, basis_ref[...])
    raw = inner[:vectors] + inner[vectors:]
    cross = contract_lanes(lhs, lhs)
    energy = (cross[:vectors, :vectors] + cross[vectors:, vectors:]) + (
        cross[:vectors, vectors:] + cross[vectors:, :vectors]
    )
    low_half = pltpu.roll(small, tile - HALF, 1)
    lane = lax.broadcasted_iota(jnp.int32, (vectors, tile), 1)
    sublane = lax.broadcasted_iota(jnp.int32, (vectors, tile), 0)
    scratch[...] = jnp.zeros_like(scratch)
    scratch[:vectors, :] = jnp.where(lane < krylov, small + low_half, 0.0)
    used = krylov + vectors
    width = HALF - used
    packet = jnp.concatenate([raw, energy, jnp.zeros((vectors, tile - used), F32)], axis=1)
    first_row = lax.axis_index("row") * each
    pieces = -(-krylov // width)
    for i in range(each):
        row = scratch[pl.ds(first_row + i, 1), :]
        for p in range(pieces):
            moved = pltpu.roll(row, (used - p * width) % tile, 1)
            here = (sublane == i * pieces + p) & (lane >= used) & (lane < HALF)
            packet = jnp.where(here, moved, packet)
    folded = jnp.where(
        lane[: vectors // 2] < HALF,
        packet[: vectors // 2],
        pltpu.roll(packet, HALF, 1)[vectors // 2 :],
    )
    packet_ref[...] = jnp.broadcast_to(folded[None], packet_ref.shape)


def tree_sum(values):
    while len(values) > 1:
        values = [sum(values[i : i + 2]) for i in range(0, len(values), 2)]
    return values[0]


def finish_kernel(
    sizes, packets_ref, applied_ref, basis_ref, new_ref, coefficients_ref, factor_ref, scratch
):
    krylov, vectors, share, each, col_count, entries = sizes
    inverse_root = 1.0 / math.sqrt(entries)
    highest = lax.Precision.HIGHEST
    devices, half, tile = packets_ref.shape
    folded = tree_sum([packets_ref[d] for d in range(devices)])
    total = jnp.concatenate([folded, pltpu.roll(folded, HALF, 1)], axis=0)
    used = krylov + vectors
    width = HALF - used
    pieces = -(-krylov // width)
    lanes = lax.broadcasted_iota(jnp.int32, (devices, tile), 1)
    for i in range(each):
        found = jnp.zeros((devices, tile), F32)
        for p in range(pieces):
            n = i * pieces + p
            start = used + (n // half) * HALF
            moved = pltpu.roll(packets_ref[:, n % half, :], (p * width - start) % tile, 1)
            found = jnp.where((lanes >= p * width) & (lanes < (p + 1) * width), moved, found)
        for d in range(devices):
            r, c = divmod(d, col_count)
            row = c * share + r * each + i
            if r * each + i < share and row < krylov:
                scratch[row : row + 1, :] = found[d : d + 1]
    correlation = scratch[:krylov, :krylov] * (1.0 / entries)
    first = total[:, :krylov] * inverse_root
    energy = total[:, krylov : krylov + vectors]
    dot = functools.partial(jnp.dot, precision=highest, preferred_element_type=F32)
    across = functools.partial(
        lax.dot_general,
        dimension_numbers=(((1,), (1,)), ((), ())),
        precision=highest,
        preferred_element_type=F32,
    )
    coefficients = first + (first - dot(first, correlation))
    coefficients_ref[...] = coefficients
    parts = jnp.concatenate(split3(coefficients * inverse_root), axis=0).astype(BF16)
    wide = jnp.dot(parts, basis_ref[...], preferred_element_type=F32)
    cleaned = applied_ref[...] - (
        wide[:vectors] + (wide[vectors : 2 * vectors] + wide[2 * vectors :])
    )
    mixed = across(first, coefficients)
    mixed_t = across(coefficients, first)
    curved = across(dot(coefficients, correlation), coefficients)
    gram = (energy - mixed - mixed_t + curved) * (1.0 / entries)
    columns = [jnp.broadcast_to(gram[:, j : j + 1], (vectors, tile)) for j in range(vectors)]
    sublane = lax.broadcasted_iota(jnp.int32, (vectors, tile), 0)
    lane = lax.broadcasted_iota(jnp.int32, (vectors, tile), 1)
    factor = jnp.zeros((vectors, tile), F32)
    length = cleaned.shape[1]
    for j in range(vectors):
        inverse = lax.rsqrt(columns[j][j : j + 1, :])
        column = jnp.where(sublane >= j, columns[j] * inverse, 0.0)
        factor = jnp.where(lane == j, column, factor)
        for k in range(j + 1, vectors):
            columns[k] = columns[k] - column * column[k : k + 1, :]
        below = jnp.where(sublane > j, column, 0.0)
        pieces = []
        for t in range(length // tile):
            piece = cleaned[:, t * tile : (t + 1) * tile]
            row = piece[j : j + 1, :] * inverse
            pieces.append(jnp.where(sublane == j, row, piece - below * row))
        cleaned = jnp.concatenate(pieces, axis=1)
    factor_ref[...] = factor[:, :vectors]
    new_ref[...] = cleaned


def shards(basis, expand, tiles, tile_rows, tile_cols):
    row_count = lax.axis_size("row")
    col_count = lax.axis_size("col")
    krylov, length = basis.shape
    tile = tiles.shape[2]
    vectors = expand.shape[1]
    rows = expand.shape[0] * vectors
    region = length // tile
    devices = row_count * col_count
    entries = length * devices
    cap = tiles.shape[1] // col_count
    extra = -(-krylov // rows)
    share = -(-krylov // col_count)
    each = -(-share // row_count)
    span = (cap + 1) * vectors
    assert krylov + vectors < HALF and share < 8 and region * vectors <= 256
    assert each * -(-krylov // (HALF - krylov - vectors)) <= vectors and cap % 2 == 0
    vmem = pl.BlockSpec(memory_space=pltpu.VMEM)
    smem = pl.BlockSpec(memory_space=pltpu.SMEM)
    hbm = pl.BlockSpec(memory_space=pltpu.HBM)

    series = pl.pallas_call(
        functools.partial(series_kernel, region, tile, extra),
        out_shape=jax.ShapeDtypeStruct((region + extra, rows, tile), BF16),
        in_specs=[hbm, hbm],
        out_specs=vmem,
        scratch_shapes=[
            pltpu.VMEM((extra * rows, tile), F32),
            pltpu.VMEM(basis.shape, BF16),
            pltpu.VMEM((rows, krylov), F32),
            pltpu.SemaphoreType.DMA((2,)),
        ],
        cost_estimate=pl.CostEstimate(flops=10**10, bytes_accessed=10**7, transcendentals=0),
        compiler_params=pltpu.CompilerParams(vmem_limit_bytes=4 << 20),
        name="series",
    )(basis, expand.reshape(rows, krylov))
    gathered = lax.all_gather(series, "row", axis=0)
    half = col_count // 2
    outgoing = jax.ShapeDtypeStruct((half, span, tile), BF16)
    mine, other = pl.pallas_call(
        functools.partial(
            tile_kernel, (row_count, region, extra, krylov, cap, vectors, share)
        ),
        out_shape=(outgoing, outgoing),
        in_specs=[smem, smem, vmem, vmem],
        out_specs=(vmem, vmem),
        scratch_shapes=[
            pltpu.VMEM((max(extra * rows, share * col_count), tile), F32),
            pltpu.VMEM((col_count, 8, tile), F32),
        ],
        compiler_params=pltpu.CompilerParams(vmem_limit_bytes=16 << 20),
        name="products",
    )(tile_cols, tile_rows, gathered, tiles)
    partner = lax.ppermute(other, "col", [(i, i ^ 1) for i in range(col_count)])
    blocks = [mine[:1], partner[:1]]
    for relative in range(half - 1, 0, -1):
        pair = jnp.stack([mine[relative], partner[relative]])
        blocks.append(
            lax.ppermute(pair, "col", [(i, i ^ (2 * relative)) for i in range(col_count)])
        )
    applied, packet = pl.pallas_call(
        functools.partial(merge_kernel, (region, krylov, cap, vectors, each)),
        out_shape=(
            jax.ShapeDtypeStruct((vectors, length), F32),
            jax.ShapeDtypeStruct((devices, vectors // 2, tile), F32),
        ),
        in_specs=[vmem] * (1 + len(blocks)),
        out_specs=(vmem, vmem),
        scratch_shapes=[pltpu.VMEM((max(8, row_count * each), tile), F32)],
        compiler_params=pltpu.CompilerParams(vmem_limit_bytes=8 << 20),
        name="merge",
    )(basis, *blocks)
    packets = lax.all_to_all(packet, ("row", "col"), 0, 0, tiled=True)
    return pl.pallas_call(
        functools.partial(finish_kernel, (krylov, vectors, share, each, col_count, entries)),
        out_shape=(
            jax.ShapeDtypeStruct((vectors, length), F32),
            jax.ShapeDtypeStruct((vectors, krylov), F32),
            jax.ShapeDtypeStruct((vectors, vectors), F32),
        ),
        in_specs=[vmem] * 3,
        out_specs=(vmem,) * 3,
        scratch_shapes=[pltpu.VMEM((share * col_count, tile), F32)],
        compiler_params=pltpu.CompilerParams(vmem_limit_bytes=4 << 20),
        name="finish",
    )(packets, applied, basis)


def solution(mesh):
    return jax.shard_map(
        shards,
        mesh=mesh,
        in_specs=(
            P(None, ("row", "col")),
            P(),
            P(None, ("row", "col"), None, None),
            P(("row", "col")),
            P(("row", "col")),
        ),
        out_specs=(P(None, ("row", "col")), P(), P()),
        check_vma=False,
    )
```

```python
import functools
import math

import jax
import jax.numpy as jnp
from jax import lax
from jax.experimental import pallas as pl
from jax.experimental.pallas import tpu as pltpu
from jax.sharding import PartitionSpec as P


F32 = jnp.float32
BF16 = jnp.bfloat16
HALF = 64


def contract_lanes(a, b):
    return lax.dot_general(a, b, (((1,), (1,)), ((), ())), preferred_element_type=F32)


def split3(value):
    high = value.astype(BF16).astype(F32)
    rest = value - high
    middle = rest.astype(BF16).astype(F32)
    return high, middle, rest - middle


def series_kernel(region, tile, extra, basis_ref, expand_ref, out_ref, scratch, here, small, sems):
    rows, krylov = expand_ref.shape
    copies = [
        pltpu.make_async_copy(basis_ref, here, sems.at[0]),
        pltpu.make_async_copy(expand_ref, small, sems.at[1]),
    ]
    for copy in copies:
        copy.start()
    scratch[...] = jnp.zeros_like(scratch)
    for copy in copies:
        copy.wait()
    basis = here[...]
    parts = jnp.concatenate(split3(small[...]), axis=0).astype(BF16)
    wide = jnp.dot(parts, basis, preferred_element_type=F32)
    series = (wide[:rows] + wide[rows : 2 * rows] + wide[2 * rows :]).astype(BF16)
    for t in range(region):
        out_ref[t] = series[:, t * tile : (t + 1) * tile]
    local = contract_lanes(basis, basis)
    high = local.astype(BF16).astype(F32)
    scratch[:krylov, :krylov] = high
    scratch[:krylov, HALF : HALF + krylov] = local - high
    for e in range(extra):
        out_ref[region + e] = scratch[e * rows : (e + 1) * rows, :].astype(BF16)


def share_correlation(sizes, gathered_ref, scratch, slices):
    row_count, region, extra, krylov, _, _, share = sizes
    rows, tile = gathered_ref.shape[2:]
    total = jnp.zeros((extra * rows, tile), F32)
    for r in range(row_count):
        total += jnp.concatenate(
            [gathered_ref[r, region + e].astype(F32) for e in range(extra)], axis=0
        )
    scratch[...] = jnp.zeros_like(scratch)
    merged = total[:krylov, :krylov] + total[:krylov, HALF : HALF + krylov]
    high = merged.astype(BF16).astype(F32)
    scratch[:krylov, :krylov] = high
    scratch[:krylov, HALF : HALF + krylov] = merged - high
    slices[...] = jnp.zeros_like(slices)
    for c in range(slices.shape[0]):
        if c * share < krylov:
            slices[c, :share, :] = scratch[c * share : (c + 1) * share, :]


def tile_kernel(sizes, core, distances, first, cols_ref, rows_ref, gathered_ref, tiles_ref, *refs):
    _, region, _, _, cap, vectors, _ = sizes
    tile = tiles_ref.shape[2]
    position = lax.axis_index("col")
    if first:
        out_ref, slices, scratch = refs
        share_correlation(sizes, gathered_ref, scratch, slices)
    else:
        slices, out_ref = refs
    lane = lax.broadcasted_iota(jnp.int32, (8, tile), 1)
    sublane = lax.broadcasted_iota(jnp.int32, (8, tile), 0)
    slot = lane // vectors
    inner = lane - slot * vectors

    def column(t):
        c = cols_ref[pl.ds(t, 1), :1][0, 0]
        r = lax.div(c, region)
        x = gathered_ref[r, c - r * region]
        return [x[m * vectors : (m + 1) * vectors] for m in range(3)]

    def weights(m, t):
        return tiles_ref[m, pl.ds(t, 2)].reshape(2 * tile, tile)

    def side(a, b):
        return jnp.concatenate([a, b], axis=1)

    def block(distance, place):
        target = (position ^ (2 * distance)) ^ core
        base = target * cap

        def store(p, out):
            pair = jnp.concatenate([out[:vectors, :tile], out[vectors:, tile:]], axis=0)
            out_ref[place, 2 * p * vectors : (2 * p + 2) * vectors, :] = pair.astype(BF16)

        pairs = []
        for p in range(cap // 2):
            t = base + 2 * p
            x0, x1 = column(t), column(t + 1)
            lhs = jnp.concatenate([side(x0[0], x0[1]), side(x1[0], x1[1])], axis=0)
            rhs = side(weights(0, t), weights(1, t))
            third = jnp.concatenate([x0[2], x1[2]], axis=0)
            pairs.append((p, contract_lanes(lhs, rhs), third, weights(2, t)))
        while len(pairs) > 1:
            (p, out_p, x_p, w_p), (q, out_q, x_q, w_q) = pairs[:2]
            pairs = pairs[2:]
            zero = jnp.zeros_like(x_p)
            lhs = jnp.concatenate([side(x_p, zero), side(zero, x_q)], axis=0)
            both = contract_lanes(lhs, side(w_p, w_q))
            store(p, out_p + both[: 2 * vectors])
            store(q, out_q + both[2 * vectors :])
        for p, out_p, x_p, w_p in pairs:
            store(p, out_p + contract_lanes(x_p, w_p))
        code = jnp.full((8, tile), -1, jnp.int32)
        for s in range(cap):
            code = jnp.where(
                slot == s, (rows_ref[pl.ds(base + s, 1), :] - target * region) * vectors + inner, code
            )
        last = jnp.where(sublane == 7, code.astype(F32), slices[target])
        out_ref[place, cap * vectors : (cap + 1) * vectors, :] = last.astype(BF16)

    for place, distance in enumerate(distances):
        block(distance, place)


def merge_kernel(sizes, basis_ref, *refs):
    region, krylov, cap, vectors, each = sizes
    blocks, (applied_ref, packet_ref, scratch) = refs[:-3], refs[-3:]
    tile = applied_ref.shape[1] // region
    total = jnp.zeros((region * vectors, tile), F32)
    small = jnp.zeros((vectors, tile), F32)
    place = lax.broadcasted_iota(jnp.int32, (region * vectors, tile), 0).astype(F32)
    span = (cap + 1) * vectors
    for ref in blocks:
        for part in range(ref.shape[0]):
            piece = ref[part]
            last = piece[cap * vectors :].astype(F32)
            small += last
            onehot = jnp.where(place == last[7:8, :], 1.0, 0.0).astype(BF16)
            total += jnp.dot(onehot[:, :span], piece, preferred_element_type=F32)
    for t in range(region):
        applied_ref[:, t * tile : (t + 1) * tile] = total[t * vectors : (t + 1) * vectors]
    applied = applied_ref[...]
    high, middle, _ = split3(applied)
    lhs = jnp.concatenate([high, middle], axis=0).astype(BF16)
    inner = contract_lanes(lhs, basis_ref[...])
    raw = inner[:vectors] + inner[vectors:]
    cross = contract_lanes(lhs, lhs)
    energy = (cross[:vectors, :vectors] + cross[vectors:, vectors:]) + (
        cross[:vectors, vectors:] + cross[vectors:, :vectors]
    )
    low_half = pltpu.roll(small, tile - HALF, 1)
    lane = lax.broadcasted_iota(jnp.int32, (vectors, tile), 1)
    sublane = lax.broadcasted_iota(jnp.int32, (vectors, tile), 0)
    scratch[...] = jnp.zeros_like(scratch)
    scratch[:vectors, :] = jnp.where(lane < krylov, small + low_half, 0.0)
    used = krylov + vectors
    width = HALF - used
    packet = jnp.concatenate([raw, energy, jnp.zeros((vectors, tile - used), F32)], axis=1)
    first_row = lax.axis_index("row") * each
    pieces = -(-krylov // width)
    for i in range(each):
        row = scratch[pl.ds(first_row + i, 1), :]
        for p in range(pieces):
            moved = pltpu.roll(row, (used - p * width) % tile, 1)
            here = (sublane == i * pieces + p) & (lane >= used) & (lane < HALF)
            packet = jnp.where(here, moved, packet)
    folded = jnp.where(
        lane[: vectors // 2] < HALF,
        packet[: vectors // 2],
        pltpu.roll(packet, HALF, 1)[vectors // 2 :],
    )
    packet_ref[...] = jnp.broadcast_to(folded[None], packet_ref.shape)


def tree_sum(values):
    while len(values) > 1:
        values = [sum(values[i : i + 2]) for i in range(0, len(values), 2)]
    return values[0]


def finish_kernel(
    sizes, packets_ref, applied_ref, basis_ref, new_ref, coefficients_ref, factor_ref, scratch
):
    krylov, vectors, share, each, col_count, entries = sizes
    inverse_root = 1.0 / math.sqrt(entries)
    highest = lax.Precision.HIGHEST
    devices, half, tile = packets_ref.shape
    folded = tree_sum([packets_ref[d] for d in range(devices)])
    total = jnp.concatenate([folded, pltpu.roll(folded, HALF, 1)], axis=0)
    used = krylov + vectors
    width = HALF - used
    pieces = -(-krylov // width)
    lanes = lax.broadcasted_iota(jnp.int32, (devices, tile), 1)
    for i in range(each):
        found = jnp.zeros((devices, tile), F32)
        for p in range(pieces):
            n = i * pieces + p
            start = used + (n // half) * HALF
            moved = pltpu.roll(packets_ref[:, n % half, :], (p * width - start) % tile, 1)
            found = jnp.where((lanes >= p * width) & (lanes < (p + 1) * width), moved, found)
        for d in range(devices):
            r, c = divmod(d, col_count)
            row = c * share + r * each + i
            if r * each + i < share and row < krylov:
                scratch[row : row + 1, :] = found[d : d + 1]
    correlation = scratch[:krylov, :krylov] * (1.0 / entries)
    first = total[:, :krylov] * inverse_root
    energy = total[:, krylov : krylov + vectors]
    dot = functools.partial(jnp.dot, precision=highest, preferred_element_type=F32)
    across = functools.partial(
        lax.dot_general,
        dimension_numbers=(((1,), (1,)), ((), ())),
        precision=highest,
        preferred_element_type=F32,
    )
    coefficients = first + (first - dot(first, correlation))
    coefficients_ref[...] = coefficients
    parts = jnp.concatenate(split3(coefficients * inverse_root), axis=0).astype(BF16)
    wide = jnp.dot(parts, basis_ref[...], preferred_element_type=F32)
    cleaned = applied_ref[...] - (
        wide[:vectors] + (wide[vectors : 2 * vectors] + wide[2 * vectors :])
    )
    mixed = across(first, coefficients)
    mixed_t = across(coefficients, first)
    curved = across(dot(coefficients, correlation), coefficients)
    gram = (energy - mixed - mixed_t + curved) * (1.0 / entries)
    columns = [jnp.broadcast_to(gram[:, j : j + 1], (vectors, tile)) for j in range(vectors)]
    sublane = lax.broadcasted_iota(jnp.int32, (vectors, tile), 0)
    lane = lax.broadcasted_iota(jnp.int32, (vectors, tile), 1)
    factor = jnp.zeros((vectors, tile), F32)
    length = cleaned.shape[1]
    for j in range(vectors):
        inverse = lax.rsqrt(columns[j][j : j + 1, :])
        column = jnp.where(sublane >= j, columns[j] * inverse, 0.0)
        factor = jnp.where(lane == j, column, factor)
        for k in range(j + 1, vectors):
            columns[k] = columns[k] - column * column[k : k + 1, :]
        below = jnp.where(sublane > j, column, 0.0)
        pieces = []
        for t in range(length // tile):
            piece = cleaned[:, t * tile : (t + 1) * tile]
            row = piece[j : j + 1, :] * inverse
            pieces.append(jnp.where(sublane == j, row, piece - below * row))
        cleaned = jnp.concatenate(pieces, axis=1)
    factor_ref[...] = factor[:, :vectors]
    new_ref[...] = cleaned


def shards(basis, expand, tiles, tile_rows, tile_cols):
    row_count = lax.axis_size("row")
    col_count = lax.axis_size("col")
    krylov, length = basis.shape
    tile = tiles.shape[2]
    vectors = expand.shape[1]
    rows = expand.shape[0] * vectors
    region = length // tile
    devices = row_count * col_count
    entries = length * devices
    cap = tiles.shape[1] // col_count
    extra = -(-krylov // rows)
    share = -(-krylov // col_count)
    each = -(-share // row_count)
    span = (cap + 1) * vectors
    assert krylov + vectors < HALF and share < 8 and region * vectors <= 256
    assert each * -(-krylov // (HALF - krylov - vectors)) <= vectors and cap % 2 == 0
    vmem = pl.BlockSpec(memory_space=pltpu.VMEM)
    smem = pl.BlockSpec(memory_space=pltpu.SMEM)
    hbm = pl.BlockSpec(memory_space=pltpu.HBM)

    series = pl.pallas_call(
        functools.partial(series_kernel, region, tile, extra),
        out_shape=jax.ShapeDtypeStruct((region + extra, rows, tile), BF16),
        in_specs=[hbm, hbm],
        out_specs=vmem,
        scratch_shapes=[
            pltpu.VMEM((extra * rows, tile), F32),
            pltpu.VMEM(basis.shape, BF16),
            pltpu.VMEM((rows, krylov), F32),
            pltpu.SemaphoreType.DMA((2,)),
        ],
        cost_estimate=pl.CostEstimate(flops=10**10, bytes_accessed=10**7, transcendentals=0),
        compiler_params=pltpu.CompilerParams(vmem_limit_bytes=4 << 20),
        name="series",
    )(pltpu.with_memory_space_constraint(basis, pltpu.HBM), pltpu.with_memory_space_constraint(expand.reshape(rows, krylov), pltpu.HBM))
    gathered = lax.all_gather(series, "row", axis=0)
    half = col_count // 2
    sizes = (row_count, region, extra, krylov, cap, vectors, share)
    table = jax.ShapeDtypeStruct((col_count, 8, tile), F32)

    wide_cols = jnp.broadcast_to(tile_cols[:, None], (tile_cols.shape[0], tile))
    wide_rows = jnp.broadcast_to(tile_rows[:, None], (tile_cols.shape[0], tile))

    def products(core, distances, *slices):
        first = not slices
        outgoing = jax.ShapeDtypeStruct((len(distances), span, tile), BF16)
        return pl.pallas_call(
            functools.partial(tile_kernel, sizes, core, distances, first),
            out_shape=(outgoing, table) if first else outgoing,
            in_specs=[vmem, vmem, vmem, vmem] + [vmem] * len(slices),
            out_specs=(vmem, vmem) if first else vmem,
            scratch_shapes=[
                pltpu.VMEM((max(extra * rows, share * col_count), tile), F32)
            ] * first,
            cost_estimate=pl.CostEstimate(
                flops=5 * 10**9, bytes_accessed=10**7, transcendentals=0
            ),
            compiler_params=pltpu.CompilerParams(vmem_limit_bytes=16 << 20),
            name="products",
        )(wide_cols, wide_rows, gathered, tiles, *slices)

    apart = tuple(range(half - 1, 0, -1))
    swap = [(i, i ^ 1) for i in range(col_count)]
    other, slices = products(1, apart + (0,))
    partner = lax.ppermute(other, "col", swap)
    mine = products(0, apart, slices)
    own = products(0, (0,), slices)
    blocks = [own, partner[half - 1 :]]
    for place, distance in enumerate(apart):
        moves = [(i, i ^ (2 * distance)) for i in range(col_count)]
        pair = jnp.stack([mine[place], partner[place]])
        blocks.append(lax.ppermute(pair, "col", moves))
    applied, packet = pl.pallas_call(
        functools.partial(merge_kernel, (region, krylov, cap, vectors, each)),
        out_shape=(
            jax.ShapeDtypeStruct((vectors, length), F32),
            jax.ShapeDtypeStruct((devices, vectors // 2, tile), F32),
        ),
        in_specs=[vmem] * (1 + len(blocks)),
        out_specs=(vmem, vmem),
        scratch_shapes=[pltpu.VMEM((max(8, row_count * each), tile), F32)],
        compiler_params=pltpu.CompilerParams(vmem_limit_bytes=8 << 20),
        name="merge",
    )(basis, *blocks)
    packets = lax.all_to_all(packet, ("row", "col"), 0, 0, tiled=True)
    return pl.pallas_call(
        functools.partial(finish_kernel, (krylov, vectors, share, each, col_count, entries)),
        out_shape=(
            jax.ShapeDtypeStruct((vectors, length), F32),
            jax.ShapeDtypeStruct((vectors, krylov), F32),
            jax.ShapeDtypeStruct((vectors, vectors), F32),
        ),
        in_specs=[vmem] * 3,
        out_specs=(vmem,) * 3,
        scratch_shapes=[pltpu.VMEM((share * col_count, tile), F32)],
        compiler_params=pltpu.CompilerParams(vmem_limit_bytes=4 << 20),
        name="finish",
    )(packets, applied, basis)


def solution(mesh):
    return jax.shard_map(
        shards,
        mesh=mesh,
        in_specs=(
            P(None, ("row", "col")),
            P(),
            P(None, ("row", "col"), None, None),
            P(("row", "col")),
            P(("row", "col")),
        ),
        out_specs=(P(None, ("row", "col")), P(), P()),
        check_vma=False,
    )
```

```python
import functools
import math

import jax
import jax.numpy as jnp
from jax import lax
from jax.experimental import pallas as pl
from jax.experimental.pallas import tpu as pltpu
from jax.sharding import PartitionSpec as P


F32 = jnp.float32
BF16 = jnp.bfloat16
HALF = 64


def contract_lanes(a, b):
    return lax.dot_general(a, b, (((1,), (1,)), ((), ())), preferred_element_type=F32)


def split3(value):
    high = value.astype(BF16).astype(F32)
    rest = value - high
    middle = rest.astype(BF16).astype(F32)
    return high, middle, rest - middle


def series_kernel(region, tile, basis_ref, expand_ref, out_ref, scratch, here, small, sems):
    rows, krylov = expand_ref.shape
    copies = [
        pltpu.make_async_copy(basis_ref, here, sems.at[0]),
        pltpu.make_async_copy(expand_ref, small, sems.at[1]),
    ]
    for copy in copies:
        copy.start()
    scratch[...] = jnp.zeros_like(scratch)
    for copy in copies:
        copy.wait()
    basis = here[...]
    parts = jnp.concatenate(split3(small[...]), axis=0).astype(BF16)
    wide = jnp.dot(parts, basis, preferred_element_type=F32)
    series = (wide[:rows] + wide[rows : 2 * rows] + wide[2 * rows :]).astype(BF16)
    for t in range(region):
        out_ref[t] = series[:, t * tile : (t + 1) * tile]
    local = contract_lanes(basis, basis)
    high = local.astype(BF16).astype(F32)
    low = local - high
    rest = krylov - rows
    corner = 2 * krylov
    scratch[:, :krylov] = high[:rows]
    scratch[:, krylov:corner] = low[:rows]
    scratch[:rest, corner : corner + rest] = high[rows:, rows:]
    scratch[:rest, corner + rest : corner + 2 * rest] = low[rows:, rows:]
    out_ref[region] = scratch[...].astype(BF16)


def share_correlation(sizes, gathered_ref, scratch, slices):
    row_count, region, krylov, _, _, share = sizes
    rows, _ = gathered_ref.shape[2:]
    rest = krylov - rows
    corner = 2 * krylov
    total = gathered_ref[0, region].astype(F32)
    for r in range(1, row_count):
        total += gathered_ref[r, region].astype(F32)
    top = total[:, :krylov] + total[:, krylov:corner]
    square = (total[:, corner : corner + rest] + total[:, corner + rest : corner + 2 * rest])[:rest]
    scratch[...] = jnp.zeros_like(scratch)
    scratch[:rows, :krylov] = top
    scratch[rows:krylov, :rows] = top.T[rows:krylov]
    scratch[rows:krylov, rows:krylov] = square
    merged = scratch[:krylov, :krylov]
    high = merged.astype(BF16).astype(F32)
    scratch[:krylov, :krylov] = high
    scratch[:krylov, HALF : HALF + krylov] = merged - high
    slices[...] = jnp.zeros_like(slices)
    for c in range(slices.shape[0]):
        if c * share < krylov:
            slices[c, :share, :] = scratch[c * share : (c + 1) * share, :]


def placed(piece, code, place):
    onehot = jnp.where(place == code, 1.0, 0.0).astype(BF16)
    return jnp.dot(onehot[:, : piece.shape[0]], piece, preferred_element_type=F32)


def tile_kernel(sizes, core, distances, kind, cols_ref, rows_ref, gathered_ref, tiles_ref, *refs):
    _, region, _, cap, vectors, _ = sizes
    tile = tiles_ref.shape[2]
    span = (cap + 1) * vectors
    position = lax.axis_index("col")
    if kind == "first":
        out_ref, slices, scratch = refs
        share_correlation(sizes, gathered_ref, scratch, slices)
    elif kind == "own":
        slices, partner_ref, total_ref, small_ref, out_ref = refs
    else:
        slices, out_ref = refs
    lane = lax.broadcasted_iota(jnp.int32, (8, tile), 1)
    sublane = lax.broadcasted_iota(jnp.int32, (8, tile), 0)
    index = lax.rem(lane + core * (tile - span), tile)
    slot = index // vectors
    inner = index - slot * vectors

    def column(t):
        c = cols_ref[pl.ds(t, 1), :1][0, 0]
        r = lax.div(c, region)
        x = gathered_ref[r, c - r * region]
        return [x[m * vectors : (m + 1) * vectors] for m in range(3)]

    def weights(m, t):
        return tiles_ref[m, pl.ds(t, 2)].reshape(2 * tile, tile)

    def side(a, b):
        return jnp.concatenate([a, b], axis=1)

    def block(distance, place):
        target = (position ^ (2 * distance)) ^ core
        base = target * cap

        def store(p, out):
            pair = jnp.concatenate([out[:vectors, :tile], out[vectors:, tile:]], axis=0)
            out_ref[place, 2 * p * vectors : (2 * p + 2) * vectors, :] = pair.astype(BF16)

        pairs = []
        for p in range(cap // 2):
            t = base + 2 * p
            x0, x1 = column(t), column(t + 1)
            lhs = jnp.concatenate([side(x0[0], x0[1]), side(x1[0], x1[1])], axis=0)
            rhs = side(weights(0, t), weights(1, t))
            third = jnp.concatenate([x0[2], x1[2]], axis=0)
            pairs.append((p, contract_lanes(lhs, rhs), third, weights(2, t)))
        while len(pairs) > 1:
            (p, out_p, x_p, w_p), (q, out_q, x_q, w_q) = pairs[:2]
            pairs = pairs[2:]
            zero = jnp.zeros_like(x_p)
            lhs = jnp.concatenate([side(x_p, zero), side(zero, x_q)], axis=0)
            both = contract_lanes(lhs, side(w_p, w_q))
            store(p, out_p + both[: 2 * vectors])
            store(q, out_q + both[2 * vectors :])
        for p, out_p, x_p, w_p in pairs:
            store(p, out_p + contract_lanes(x_p, w_p))
        code = jnp.full((8, tile), -1, jnp.int32)
        for s in range(cap):
            code = jnp.where(
                slot == s, (rows_ref[pl.ds(base + s, 1), :] - target * region) * vectors + inner, code
            )
        last = jnp.where(sublane == 7, code.astype(F32), slices[target])
        out_ref[place, cap * vectors : (cap + 1) * vectors, :] = last.astype(BF16)

    for place, distance in enumerate(distances):
        block(distance, place)
    if kind == "own":
        place = lax.broadcasted_iota(jnp.int32, (region * vectors, tile), 0).astype(F32)
        total = jnp.zeros((region * vectors, tile), F32)
        small = jnp.zeros((vectors, tile), F32)
        for piece, shift in ((out_ref[0], 0), (partner_ref[partner_ref.shape[0] - 1], tile - span)):
            last = piece[cap * vectors :].astype(F32)
            small += last
            code = pltpu.roll(last, shift, 1) if shift else last
            total += placed(piece, code[7:8, :], place)
        total_ref[...] = total
        small_ref[...] = small


def merge_kernel(sizes, basis_ref, total_ref, small_ref, *refs):
    region, krylov, cap, vectors, each = sizes
    blocks, (applied_ref, packet_ref, scratch) = refs[:-3], refs[-3:]
    tile = applied_ref.shape[1] // region
    total = total_ref[...]
    small = small_ref[...]
    place = lax.broadcasted_iota(jnp.int32, (region * vectors, 2 * tile), 0).astype(F32)
    span = (cap + 1) * vectors
    row_lane = lax.broadcasted_iota(jnp.int32, (1, tile), 1)
    for ref in blocks:
        piece = ref[...]
        near = piece[cap * vectors : span].astype(F32)
        far = piece[span + cap * vectors :].astype(F32)
        small += near + far
        code = jnp.where(row_lane < span, near[7:8, :], far[7:8, :])
        total += placed(piece, jnp.concatenate([code, far[7:8, :]], axis=1), place)
    for t in range(region):
        applied_ref[:, t * tile : (t + 1) * tile] = total[t * vectors : (t + 1) * vectors]
    applied = applied_ref[...]
    high, middle, _ = split3(applied)
    lhs = jnp.concatenate([high, middle], axis=0).astype(BF16)
    inner = contract_lanes(lhs, basis_ref[...])
    raw = inner[:vectors] + inner[vectors:]
    cross = contract_lanes(lhs, lhs)
    energy = (cross[:vectors, :vectors] + cross[vectors:, vectors:]) + (
        cross[:vectors, vectors:] + cross[vectors:, :vectors]
    )
    low_half = pltpu.roll(small, tile - HALF, 1)
    lane = lax.broadcasted_iota(jnp.int32, (vectors, tile), 1)
    sublane = lax.broadcasted_iota(jnp.int32, (vectors, tile), 0)
    scratch[...] = jnp.zeros_like(scratch)
    scratch[:vectors, :] = jnp.where(lane < krylov, small + low_half, 0.0)
    used = krylov + vectors
    width = HALF - used
    packet = jnp.concatenate([raw, energy, jnp.zeros((vectors, tile - used), F32)], axis=1)
    first_row = lax.axis_index("row") * each
    pieces = -(-krylov // width)
    for i in range(each):
        row = scratch[pl.ds(first_row + i, 1), :]
        for p in range(pieces):
            moved = pltpu.roll(row, (used - p * width) % tile, 1)
            here = (sublane == i * pieces + p) & (lane >= used) & (lane < HALF)
            packet = jnp.where(here, moved, packet)
    folded = jnp.where(
        lane[: vectors // 2] < HALF,
        packet[: vectors // 2],
        pltpu.roll(packet, HALF, 1)[vectors // 2 :],
    )
    packet_ref[...] = jnp.broadcast_to(folded[None], packet_ref.shape)


def tree_sum(values):
    while len(values) > 1:
        values = [sum(values[i : i + 2]) for i in range(0, len(values), 2)]
    return values[0]


def finish_kernel(
    sizes, packets_ref, applied_ref, basis_ref, new_ref, coefficients_ref, factor_ref, scratch
):
    krylov, vectors, share, each, col_count, entries = sizes
    inverse_root = 1.0 / math.sqrt(entries)
    highest = lax.Precision.HIGHEST
    devices, half, tile = packets_ref.shape
    folded = tree_sum([packets_ref[d] for d in range(devices)])
    total = jnp.concatenate([folded, pltpu.roll(folded, HALF, 1)], axis=0)
    used = krylov + vectors
    width = HALF - used
    pieces = -(-krylov // width)
    lanes = lax.broadcasted_iota(jnp.int32, (devices, tile), 1)
    for i in range(each):
        found = jnp.zeros((devices, tile), F32)
        for p in range(pieces):
            n = i * pieces + p
            start = used + (n // half) * HALF
            moved = pltpu.roll(packets_ref[:, n % half, :], (p * width - start) % tile, 1)
            found = jnp.where((lanes >= p * width) & (lanes < (p + 1) * width), moved, found)
        for d in range(devices):
            r, c = divmod(d, col_count)
            row = c * share + r * each + i
            if r * each + i < share and row < krylov:
                scratch[row : row + 1, :] = found[d : d + 1]
    correlation = scratch[:krylov, :krylov] * (1.0 / entries)
    first = total[:, :krylov] * inverse_root
    energy = total[:, krylov : krylov + vectors]
    dot = functools.partial(jnp.dot, precision=highest, preferred_element_type=F32)
    across = functools.partial(
        lax.dot_general,
        dimension_numbers=(((1,), (1,)), ((), ())),
        precision=highest,
        preferred_element_type=F32,
    )
    coefficients = first + (first - dot(first, correlation))
    coefficients_ref[...] = coefficients
    parts = jnp.concatenate(split3(coefficients * inverse_root), axis=0).astype(BF16)
    wide = jnp.dot(parts, basis_ref[...], preferred_element_type=F32)
    cleaned = applied_ref[...] - (
        wide[:vectors] + (wide[vectors : 2 * vectors] + wide[2 * vectors :])
    )
    mixed = across(first, coefficients)
    mixed_t = across(coefficients, first)
    curved = across(dot(coefficients, correlation), coefficients)
    gram = (energy - mixed - mixed_t + curved) * (1.0 / entries)
    columns = [jnp.broadcast_to(gram[:, j : j + 1], (vectors, tile)) for j in range(vectors)]
    sublane = lax.broadcasted_iota(jnp.int32, (vectors, tile), 0)
    lane = lax.broadcasted_iota(jnp.int32, (vectors, tile), 1)
    factor = jnp.zeros((vectors, tile), F32)
    length = cleaned.shape[1]
    for j in range(vectors):
        inverse = lax.rsqrt(columns[j][j : j + 1, :])
        column = jnp.where(sublane >= j, columns[j] * inverse, 0.0)
        factor = jnp.where(lane == j, column, factor)
        for k in range(j + 1, vectors):
            columns[k] = columns[k] - column * column[k : k + 1, :]
        below = jnp.where(sublane > j, column, 0.0)
        pieces = []
        for t in range(length // tile):
            piece = cleaned[:, t * tile : (t + 1) * tile]
            row = piece[j : j + 1, :] * inverse
            pieces.append(jnp.where(sublane == j, row, piece - below * row))
        cleaned = jnp.concatenate(pieces, axis=1)
    factor_ref[...] = factor[:, :vectors]
    new_ref[...] = cleaned


def shards(basis, expand, tiles, tile_rows, tile_cols):
    row_count = lax.axis_size("row")
    col_count = lax.axis_size("col")
    krylov, length = basis.shape
    tile = tiles.shape[2]
    vectors = expand.shape[1]
    rows = expand.shape[0] * vectors
    region = length // tile
    devices = row_count * col_count
    entries = length * devices
    cap = tiles.shape[1] // col_count
    share = -(-krylov // col_count)
    each = -(-share // row_count)
    span = (cap + 1) * vectors
    assert krylov + vectors < HALF and share < 8 and region * vectors <= 256
    assert each * -(-krylov // (HALF - krylov - vectors)) <= vectors and cap % 2 == 0
    assert rows < krylov <= 2 * rows and 4 * krylov - 2 * rows <= tile
    vmem = pl.BlockSpec(memory_space=pltpu.VMEM)
    hbm = pl.BlockSpec(memory_space=pltpu.HBM)

    series = pl.pallas_call(
        functools.partial(series_kernel, region, tile),
        out_shape=jax.ShapeDtypeStruct((region + 1, rows, tile), BF16),
        in_specs=[hbm, hbm],
        out_specs=vmem,
        scratch_shapes=[
            pltpu.VMEM((rows, tile), F32),
            pltpu.VMEM(basis.shape, BF16),
            pltpu.VMEM((rows, krylov), F32),
            pltpu.SemaphoreType.DMA((2,)),
        ],
        cost_estimate=pl.CostEstimate(flops=10**10, bytes_accessed=10**7, transcendentals=0),
        compiler_params=pltpu.CompilerParams(vmem_limit_bytes=4 << 20),
        name="series",
    )(
        pltpu.with_memory_space_constraint(basis, pltpu.HBM),
        pltpu.with_memory_space_constraint(expand.reshape(rows, krylov), pltpu.HBM),
    )
    gathered = lax.all_gather(series, "row", axis=0)
    half = col_count // 2
    sizes = (row_count, region, krylov, cap, vectors, share)
    wide_cols = jnp.broadcast_to(tile_cols[:, None], (tile_cols.shape[0], tile))
    wide_rows = jnp.broadcast_to(tile_rows[:, None], (tile_rows.shape[0], tile))

    def products(kind, core, distances, *rest):
        outgoing = (len(distances), span, tile)
        shapes = {
            "first": ((outgoing, BF16), ((col_count, 8, tile), F32)),
            "mine": ((outgoing, BF16),),
            "own": (((region * vectors, tile), F32), ((vectors, tile), F32)),
        }[kind]
        scratch = {
            "first": [pltpu.VMEM((max(krylov, share * col_count), tile), F32)],
            "mine": [],
            "own": [pltpu.VMEM(outgoing, BF16)],
        }[kind]
        return pl.pallas_call(
            functools.partial(tile_kernel, sizes, core, distances, kind),
            out_shape=tuple(jax.ShapeDtypeStruct(*shape) for shape in shapes),
            in_specs=[vmem] * (4 + len(rest)),
            out_specs=(vmem,) * len(shapes),
            scratch_shapes=scratch,
            cost_estimate=pl.CostEstimate(
                flops=5 * 10**9, bytes_accessed=10**7, transcendentals=0
            ),
            compiler_params=pltpu.CompilerParams(vmem_limit_bytes=16 << 20),
            name="products",
        )(wide_cols, wide_rows, gathered, tiles, *rest)

    apart = tuple(range(half - 1, 0, -1))
    swap = [(i, i ^ 1) for i in range(col_count)]
    other, slices = products("first", 1, apart + (0,))
    partner = lax.ppermute(other, "col", swap)
    (mine,) = products("mine", 0, apart, slices)
    blocks = list(products("own", 0, (0,), slices, partner))
    for place, distance in enumerate(apart):
        moves = [(i, i ^ (2 * distance)) for i in range(col_count)]
        pair = jnp.concatenate([mine[place], partner[place]], axis=0)
        blocks.append(lax.ppermute(pair, "col", moves))
    applied, packet = pl.pallas_call(
        functools.partial(merge_kernel, (region, krylov, cap, vectors, each)),
        out_shape=(
            jax.ShapeDtypeStruct((vectors, length), F32),
            jax.ShapeDtypeStruct((devices, vectors // 2, tile), F32),
        ),
        in_specs=[vmem] * (1 + len(blocks)),
        out_specs=(vmem, vmem),
        scratch_shapes=[pltpu.VMEM((max(8, row_count * each), tile), F32)],
        compiler_params=pltpu.CompilerParams(vmem_limit_bytes=8 << 20),
        name="merge",
    )(basis, *blocks)
    packets = lax.all_to_all(packet, ("row", "col"), 0, 0, tiled=True)
    return pl.pallas_call(
        functools.partial(finish_kernel, (krylov, vectors, share, each, col_count, entries)),
        out_shape=(
            jax.ShapeDtypeStruct((vectors, length), F32),
            jax.ShapeDtypeStruct((vectors, krylov), F32),
            jax.ShapeDtypeStruct((vectors, vectors), F32),
        ),
        in_specs=[vmem] * 3,
        out_specs=(vmem,) * 3,
        scratch_shapes=[pltpu.VMEM((share * col_count, tile), F32)],
        compiler_params=pltpu.CompilerParams(vmem_limit_bytes=4 << 20),
        name="finish",
    )(packets, applied, basis)


def solution(mesh):
    return jax.shard_map(
        shards,
        mesh=mesh,
        in_specs=(
            P(None, ("row", "col")),
            P(),
            P(None, ("row", "col"), None, None),
            P(("row", "col")),
            P(("row", "col")),
        ),
        out_specs=(P(None, ("row", "col")), P(), P()),
        check_vma=False,
    )
```

```python
import functools
import math

import jax
import jax.numpy as jnp
from jax import lax
from jax.experimental import pallas as pl
from jax.experimental.pallas import tpu as pltpu
from jax.sharding import PartitionSpec as P


F32 = jnp.float32
BF16 = jnp.bfloat16
HALF = 64


def contract_lanes(a, b):
    return lax.dot_general(a, b, (((1,), (1,)), ((), ())), preferred_element_type=F32)


def split3(value):
    high = value.astype(BF16).astype(F32)
    rest = value - high
    middle = rest.astype(BF16).astype(F32)
    return high, middle, rest - middle


def series_kernel(
    region, tile, basis_ref, expand_ref, cols_ref, rows_ref, out_ref, *refs
):
    tables, (scratch, here, small, lists, sems) = refs[:2], refs[2:]
    rows, krylov = expand_ref.shape
    groups = basis_ref.shape[0] // 8
    copies = [pltpu.make_async_copy(expand_ref, small, sems.at[groups])]
    copies.append(pltpu.make_async_copy(cols_ref, lists.at[0], sems.at[groups + 1]))
    copies.append(pltpu.make_async_copy(rows_ref, lists.at[1], sems.at[groups + 2]))
    for g in range(groups):
        part = pl.ds(8 * g, 8)
        copies.append(pltpu.make_async_copy(basis_ref.at[part], here.at[part], sems.at[g]))
    for copy in copies:
        copy.start()
    scratch[...] = jnp.zeros_like(scratch)
    for copy in copies:
        copy.wait()
    basis = here[...]
    parts = jnp.concatenate(split3(small[...])[:2], axis=0).astype(BF16)
    wide = jnp.dot(parts, basis, preferred_element_type=F32)
    series = (wide[:rows] + wide[rows:]).astype(BF16)
    for t in range(region):
        out_ref[t] = series[:, t * tile : (t + 1) * tile]
    local = contract_lanes(basis, basis)
    high = local.astype(BF16).astype(F32)
    low = local - high
    rest = krylov - rows
    corner = 2 * krylov
    scratch[:, :krylov] = high[:rows]
    scratch[:, krylov:corner] = low[:rows]
    scratch[:rest, corner : corner + rest] = high[rows:, rows:]
    scratch[:rest, corner + rest : corner + 2 * rest] = low[rows:, rows:]
    out_ref[region] = scratch[...].astype(BF16)
    for k, table in enumerate(tables):
        spread = jnp.broadcast_to(lists[k].astype(F32), (tile, lists.shape[2]))
        table[...] = spread.T.astype(jnp.int32)


def share_correlation(sizes, gathered_ref, scratch, slices):
    row_count, region, krylov, _, _, share = sizes
    rows, _ = gathered_ref.shape[2:]
    rest = krylov - rows
    corner = 2 * krylov
    total = gathered_ref[0, region].astype(F32)
    for r in range(1, row_count):
        total += gathered_ref[r, region].astype(F32)
    top = total[:, :krylov] + total[:, krylov:corner]
    square = (total[:, corner : corner + rest] + total[:, corner + rest : corner + 2 * rest])[:rest]
    scratch[...] = jnp.zeros_like(scratch)
    scratch[:rows, :krylov] = top
    scratch[rows:krylov, :rows] = top.T[rows:krylov]
    scratch[rows:krylov, rows:krylov] = square
    merged = scratch[:krylov, :krylov]
    high = merged.astype(BF16).astype(F32)
    scratch[:krylov, :krylov] = high
    scratch[:krylov, HALF : HALF + krylov] = merged - high
    slices[...] = jnp.zeros_like(slices)
    for c in range(slices.shape[0]):
        if c * share < krylov:
            slices[c, :share, :] = scratch[c * share : (c + 1) * share, :]


def placed(piece, code, place):
    onehot = jnp.where(place == code, 1.0, 0.0).astype(BF16)
    return jnp.dot(onehot[:, : piece.shape[0]], piece, preferred_element_type=F32)


def tile_kernel(sizes, groups, first, cols_ref, rows_ref, gathered_ref, tiles_ref, *refs):
    refs, turned = refs[:-1], refs[-1]
    used = []
    _, region, _, cap, vectors, _ = sizes
    tile = tiles_ref.shape[2]
    span = (cap + 1) * vectors
    position = lax.axis_index("col")
    if first:
        slices, scratch = refs[-2:]
        out_refs = refs[:-2]
        share_correlation(sizes, gathered_ref, scratch, slices)
    else:
        slices, out_refs = refs[0], refs[1:]
    lane = lax.broadcasted_iota(jnp.int32, (8, tile), 1)
    sublane = lax.broadcasted_iota(jnp.int32, (8, tile), 0)

    def column(t):
        c = cols_ref[pl.ds(t, 1), :1][0, 0]
        r = lax.div(c, region)
        x = gathered_ref[r, c - r * region]
        return [x[m * vectors : (m + 1) * vectors] for m in range(3)]

    def weights(m, t):
        return tiles_ref[m, pl.ds(t, 2)].reshape(2 * tile, tile)

    def through(lhs, rhs):
        slot = len(used)
        used.append(slot)
        turned[slot] = rhs.T
        return jnp.dot(lhs, turned[slot], preferred_element_type=F32)

    def side(a, b):
        return jnp.concatenate([a, b], axis=1)

    def block(core, distance, out_ref, place):
        target = (position ^ (2 * distance)) ^ core
        index = lax.rem(lane + core * (tile - span), tile)
        slot = index // vectors
        inner = index - slot * vectors
        base = target * cap

        def store(p, out):
            pair = jnp.concatenate([out[:vectors, :tile], out[vectors:, tile:]], axis=0)
            out_ref[place, 2 * p * vectors : (2 * p + 2) * vectors, :] = pair.astype(BF16)

        pairs = []
        for p in range(cap // 2):
            t = base + 2 * p
            x0, x1 = column(t), column(t + 1)
            lhs = jnp.concatenate([side(x0[0], x0[1]), side(x1[0], x1[1])], axis=0)
            rhs = side(weights(0, t), weights(1, t))
            third = jnp.concatenate([x0[2], x1[2]], axis=0)
            out = through(lhs, rhs)
            pairs.append((p, out, third, weights(2, t)))
        while len(pairs) > 1:
            (p, out_p, x_p, w_p), (q, out_q, x_q, w_q) = pairs[:2]
            pairs = pairs[2:]
            zero = jnp.zeros_like(x_p)
            lhs = jnp.concatenate([side(x_p, zero), side(zero, x_q)], axis=0)
            both = contract_lanes(lhs, side(w_p, w_q))
            store(p, out_p + both[: 2 * vectors])
            store(q, out_q + both[2 * vectors :])
        for p, out_p, x_p, w_p in pairs:
            store(p, out_p + contract_lanes(x_p, w_p))
        code = jnp.full((8, tile), -1, jnp.int32)
        for s in range(cap):
            code = jnp.where(
                slot == s, (rows_ref[pl.ds(base + s, 1), :] - target * region) * vectors + inner, code
            )
        last = jnp.where(sublane == 7, code.astype(F32), slices[target])
        out_ref[place, cap * vectors : (cap + 1) * vectors, :] = last.astype(BF16)

    for group, out_ref in zip(groups, out_refs):
        for place, (core, distance) in enumerate(group):
            block(core, distance, out_ref, place)


def own_kernel(sizes, own_ref, partner_ref, total_ref, small_ref):
    _, _, _, cap, vectors, _ = sizes
    tile = total_ref.shape[1]
    span = (cap + 1) * vectors
    place = lax.broadcasted_iota(jnp.int32, total_ref.shape, 0).astype(F32)
    total = jnp.zeros(total_ref.shape, F32)
    small = jnp.zeros(small_ref.shape, F32)
    for piece, shift in ((own_ref[0], 0), (partner_ref[0], tile - span)):
        last = piece[cap * vectors :].astype(F32)
        small += last
        code = pltpu.roll(last, shift, 1) if shift else last
        total += placed(piece, code[7:8, :], place)
    total_ref[...] = total
    small_ref[...] = small


def merge_kernel(sizes, basis_ref, total_ref, small_ref, *refs):
    region, krylov, cap, vectors, each = sizes
    blocks, (applied_ref, packet_ref, scratch) = refs[:-3], refs[-3:]
    tile = applied_ref.shape[1] // region
    total = total_ref[...]
    small = small_ref[...]
    place = lax.broadcasted_iota(jnp.int32, (region * vectors, 2 * tile), 0).astype(F32)
    span = (cap + 1) * vectors
    row_lane = lax.broadcasted_iota(jnp.int32, (1, tile), 1)
    for ref in blocks:
        piece = ref[...]
        near = piece[cap * vectors : span].astype(F32)
        far = piece[span + cap * vectors :].astype(F32)
        small += near + far
        code = jnp.where(row_lane < span, near[7:8, :], far[7:8, :])
        total += placed(piece, jnp.concatenate([code, far[7:8, :]], axis=1), place)
    for t in range(region):
        applied_ref[:, t * tile : (t + 1) * tile] = total[t * vectors : (t + 1) * vectors]
    applied = applied_ref[...]
    high, middle, _ = split3(applied)
    lhs = jnp.concatenate([high, middle], axis=0).astype(BF16)
    inner = contract_lanes(lhs, basis_ref[...])
    raw = inner[:vectors] + inner[vectors:]
    cross = contract_lanes(lhs, lhs)
    energy = (cross[:vectors, :vectors] + cross[vectors:, vectors:]) + (
        cross[:vectors, vectors:] + cross[vectors:, :vectors]
    )
    low_half = pltpu.roll(small, tile - HALF, 1)
    lane = lax.broadcasted_iota(jnp.int32, (vectors, tile), 1)
    sublane = lax.broadcasted_iota(jnp.int32, (vectors, tile), 0)
    scratch[...] = jnp.zeros_like(scratch)
    scratch[:vectors, :] = jnp.where(lane < krylov, small + low_half, 0.0)
    used = krylov + vectors
    width = HALF - used
    packet = jnp.concatenate([raw, energy, jnp.zeros((vectors, tile - used), F32)], axis=1)
    first_row = lax.axis_index("row") * each
    pieces = -(-krylov // width)
    for i in range(each):
        row = scratch[pl.ds(first_row + i, 1), :]
        for p in range(pieces):
            moved = pltpu.roll(row, (used - p * width) % tile, 1)
            here = (sublane == i * pieces + p) & (lane >= used) & (lane < HALF)
            packet = jnp.where(here, moved, packet)
    folded = jnp.where(
        lane[: vectors // 2] < HALF,
        packet[: vectors // 2],
        pltpu.roll(packet, HALF, 1)[vectors // 2 :],
    )
    packet_ref[...] = jnp.broadcast_to(folded[None], packet_ref.shape)


def tree_sum(values):
    while len(values) > 1:
        values = [sum(values[i : i + 2]) for i in range(0, len(values), 2)]
    return values[0]


def finish_kernel(
    sizes, packets_ref, applied_ref, basis_ref, new_ref, coefficients_ref, factor_ref, scratch
):
    krylov, vectors, share, each, col_count, entries = sizes
    inverse_root = 1.0 / math.sqrt(entries)
    devices, half, tile = packets_ref.shape
    folded = tree_sum([packets_ref[d] for d in range(devices)])
    total = jnp.concatenate([folded, pltpu.roll(folded, HALF, 1)], axis=0)
    used = krylov + vectors
    width = HALF - used
    pieces = -(-krylov // width)
    lanes = lax.broadcasted_iota(jnp.int32, (devices, tile), 1)
    for i in range(each):
        found = jnp.zeros((devices, tile), F32)
        for p in range(pieces):
            n = i * pieces + p
            start = used + (n // half) * HALF
            moved = pltpu.roll(packets_ref[:, n % half, :], (p * width - start) % tile, 1)
            found = jnp.where((lanes >= p * width) & (lanes < (p + 1) * width), moved, found)
        for d in range(devices):
            r, c = divmod(d, col_count)
            row = c * share + r * each + i
            if r * each + i < share and row < krylov:
                scratch[row : row + 1, :] = found[d : d + 1]
    correlation = scratch[:krylov, :krylov] * (1.0 / entries)
    first = total[:, :krylov] * inverse_root
    energy = total[:, krylov : krylov + vectors]
    corr_high = correlation.astype(BF16)
    corr_low = (correlation - corr_high.astype(F32)).astype(BF16)

    def halves(value):
        high = value.astype(BF16).astype(F32)
        return high.astype(BF16), jnp.concatenate([high, value - high], axis=0).astype(BF16)

    def times_correlation(value):
        high, both = halves(value)
        main = jnp.dot(both, corr_high, preferred_element_type=F32)
        rest = jnp.dot(high, corr_low, preferred_element_type=F32)
        return main[:vectors] + (main[vectors:] + rest)

    coefficients = first + (first - times_correlation(first))
    coefficients_ref[...] = coefficients
    _, parts = halves(coefficients * inverse_root)
    wide = jnp.dot(parts, basis_ref[...], preferred_element_type=F32)
    cleaned = applied_ref[...] - (wide[:vectors] + wide[vectors:])
    coef_high, coef_both = halves(coefficients)
    high, both = halves(times_correlation(coefficients) - 2.0 * first)
    main = contract_lanes(both, coef_high)
    rest = contract_lanes(high, coef_both[vectors:])
    gram = (energy + main[:vectors] + (main[vectors:] + rest)) * (1.0 / entries)
    columns = [jnp.broadcast_to(gram[:, j : j + 1], (vectors, tile)) for j in range(vectors)]
    sublane = lax.broadcasted_iota(jnp.int32, (vectors, tile), 0)
    lane = lax.broadcasted_iota(jnp.int32, (vectors, tile), 1)
    factor = jnp.zeros((vectors, tile), F32)
    length = cleaned.shape[1]
    for j in range(vectors):
        inverse = lax.rsqrt(columns[j][j : j + 1, :])
        column = jnp.where(sublane >= j, columns[j] * inverse, 0.0)
        factor = jnp.where(lane == j, column, factor)
        for k in range(j + 1, vectors):
            columns[k] = columns[k] - column * column[k : k + 1, :]
        below = jnp.where(sublane > j, column, 0.0)
        pieces = []
        for t in range(length // tile):
            piece = cleaned[:, t * tile : (t + 1) * tile]
            row = piece[j : j + 1, :] * inverse
            pieces.append(jnp.where(sublane == j, row, piece - below * row))
        cleaned = jnp.concatenate(pieces, axis=1)
    factor_ref[...] = factor[:, :vectors]
    new_ref[...] = cleaned


def shards(basis, expand, tiles, tile_rows, tile_cols):
    row_count = lax.axis_size("row")
    col_count = lax.axis_size("col")
    krylov, length = basis.shape
    tile = tiles.shape[2]
    vectors = expand.shape[1]
    rows = expand.shape[0] * vectors
    region = length // tile
    devices = row_count * col_count
    entries = length * devices
    cap = tiles.shape[1] // col_count
    share = -(-krylov // col_count)
    each = -(-share // row_count)
    span = (cap + 1) * vectors
    assert krylov + vectors < HALF and share < 8 and region * vectors <= 256
    assert each * -(-krylov // (HALF - krylov - vectors)) <= vectors and cap % 2 == 0
    assert rows < krylov <= 2 * rows and 4 * krylov - 2 * rows <= tile
    vmem = pl.BlockSpec(memory_space=pltpu.VMEM)
    hbm = pl.BlockSpec(memory_space=pltpu.HBM)

    count = tile_cols.shape[0]
    index_table = jax.ShapeDtypeStruct((count, tile), jnp.int32)
    series, wide_cols, wide_rows = pl.pallas_call(
        functools.partial(series_kernel, region, tile),
        out_shape=(
            jax.ShapeDtypeStruct((region + 1, rows, tile), BF16),
            index_table,
            index_table,
        ),
        in_specs=[hbm] * 4,
        out_specs=(vmem,) * 3,
        scratch_shapes=[
            pltpu.VMEM((rows, tile), F32),
            pltpu.VMEM(basis.shape, BF16),
            pltpu.VMEM((rows, krylov), F32),
            pltpu.VMEM((2, 1, count), jnp.int32),
            pltpu.SemaphoreType.DMA((krylov // 8 + 3,)),
        ],
        cost_estimate=pl.CostEstimate(flops=10**10, bytes_accessed=10**7, transcendentals=0),
        compiler_params=pltpu.CompilerParams(vmem_limit_bytes=4 << 20),
        name="series",
    )(
        *(
            pltpu.with_memory_space_constraint(value, pltpu.HBM)
            for value in (
                basis,
                expand.reshape(rows, krylov),
                tile_cols.reshape(1, count),
                tile_rows.reshape(1, count),
            )
        )
    )
    gathered = lax.all_gather(series, "row", axis=0)
    half = col_count // 2
    sizes = (row_count, region, krylov, cap, vectors, share)

    def products(groups, *slices):
        first = not slices
        shapes = [((len(group), span, tile), BF16) for group in groups]
        shapes += [((col_count, 8, tile), F32)] * first
        return pl.pallas_call(
            functools.partial(tile_kernel, sizes, groups, first),
            out_shape=tuple(jax.ShapeDtypeStruct(*shape) for shape in shapes),
            in_specs=[vmem] * (4 + len(slices)),
            out_specs=(vmem,) * len(shapes),
            scratch_shapes=[pltpu.VMEM((max(krylov, share * col_count), tile), F32)] * first
            + [pltpu.VMEM((9 * max(1, sum(map(len, groups))), 2 * tile, 2 * tile), BF16)],
            cost_estimate=pl.CostEstimate(
                flops=5 * 10**9, bytes_accessed=10**7, transcendentals=0
            ),
            compiler_params=pltpu.CompilerParams(vmem_limit_bytes=16 << 20),
            name="products",
        )(wide_cols, wide_rows, gathered, tiles, *slices)

    apart = tuple(range(half - 1, 0, -1))
    far = apart
    swap = [(i, i ^ 1) for i in range(col_count)]
    other, slices = products((tuple((1, d) for d in apart),))
    partner = lax.ppermute(other, "col", swap)
    (mine_far,) = products((tuple((0, d) for d in far),), slices)
    other_here, own = products((((1, 0),), ((0, 0),)), slices)
    partner_here = lax.ppermute(other_here, "col", swap)
    blocks = list(
        pl.pallas_call(
            functools.partial(own_kernel, sizes),
            out_shape=(
                jax.ShapeDtypeStruct((region * vectors, tile), F32),
                jax.ShapeDtypeStruct((vectors, tile), F32),
            ),
            in_specs=[vmem] * 2,
            out_specs=(vmem,) * 2,
            cost_estimate=pl.CostEstimate(flops=5 * 10**8, bytes_accessed=10**6, transcendentals=0),
            compiler_params=pltpu.CompilerParams(vmem_limit_bytes=8 << 20),
            name="own",
        )(own, partner_here)
    )
    for distances, mine in ((far, mine_far),):
        for place, distance in enumerate(distances):
            moves = [(i, i ^ (2 * distance)) for i in range(col_count)]
            pair = jnp.concatenate([mine[place], partner[apart.index(distance)]], axis=0)
            blocks.append(lax.ppermute(pair, "col", moves))
    applied, packet = pl.pallas_call(
        functools.partial(merge_kernel, (region, krylov, cap, vectors, each)),
        out_shape=(
            jax.ShapeDtypeStruct((vectors, length), F32),
            jax.ShapeDtypeStruct((devices, vectors // 2, tile), F32),
        ),
        in_specs=[vmem] * (1 + len(blocks)),
        out_specs=(vmem, vmem),
        scratch_shapes=[pltpu.VMEM((max(8, row_count * each), tile), F32)],
        compiler_params=pltpu.CompilerParams(vmem_limit_bytes=8 << 20),
        name="merge",
    )(basis, *blocks)
    packets = lax.all_to_all(packet, ("row", "col"), 0, 0, tiled=True)
    return pl.pallas_call(
        functools.partial(finish_kernel, (krylov, vectors, share, each, col_count, entries)),
        out_shape=(
            jax.ShapeDtypeStruct((vectors, length), F32),
            jax.ShapeDtypeStruct((vectors, krylov), F32),
            jax.ShapeDtypeStruct((vectors, vectors), F32),
        ),
        in_specs=[vmem] * 3,
        out_specs=(vmem,) * 3,
        scratch_shapes=[pltpu.VMEM((share * col_count, tile), F32)],
        compiler_params=pltpu.CompilerParams(vmem_limit_bytes=4 << 20),
        name="finish",
    )(packets, applied, basis)


def solution(mesh):
    return jax.shard_map(
        shards,
        mesh=mesh,
        in_specs=(
            P(None, ("row", "col")),
            P(),
            P(None, ("row", "col"), None, None),
            P(("row", "col")),
            P(("row", "col")),
        ),
        out_specs=(P(None, ("row", "col")), P(), P()),
        check_vma=False,
    )
```

```python
import functools
import math

import jax
import jax.numpy as jnp
from jax import lax
from jax.experimental import pallas as pl
from jax.experimental.pallas import tpu as pltpu
from jax.sharding import PartitionSpec as P


F32 = jnp.float32
BF16 = jnp.bfloat16
HALF = 64


def contract_lanes(a, b):
    return lax.dot_general(a, b, (((1,), (1,)), ((), ())), preferred_element_type=F32)


def split3(value):
    high = value.astype(BF16).astype(F32)
    rest = value - high
    middle = rest.astype(BF16).astype(F32)
    return high, middle, rest - middle


def series_kernel(
    region, tile, basis_ref, expand_ref, cols_ref, rows_ref, out_ref, local_ref, *refs
):
    tables, (here, small, lists, sems) = refs[:2], refs[2:]
    rows, krylov = expand_ref.shape
    groups = basis_ref.shape[0] // 8
    copies = [pltpu.make_async_copy(expand_ref, small, sems.at[groups])]
    copies.append(pltpu.make_async_copy(cols_ref, lists.at[0], sems.at[groups + 1]))
    copies.append(pltpu.make_async_copy(rows_ref, lists.at[1], sems.at[groups + 2]))
    for g in range(groups):
        part = pl.ds(8 * g, 8)
        copies.append(pltpu.make_async_copy(basis_ref.at[part], here.at[part], sems.at[g]))
    for copy in copies:
        copy.start()
    local_ref[...] = jnp.zeros_like(local_ref)
    for copy in copies:
        copy.wait()
    basis = here[...]
    parts = jnp.concatenate(split3(small[...])[:2], axis=0).astype(BF16)
    wide = jnp.dot(parts, basis, preferred_element_type=F32)
    series = (wide[:rows] + wide[rows:]).astype(BF16)
    for t in range(region):
        out_ref[t] = series[:, t * tile : (t + 1) * tile]
    krylov = basis.shape[0]
    local_ref[:, :krylov] = contract_lanes(basis, basis)
    for k, table in enumerate(tables):
        spread = jnp.broadcast_to(lists[k].astype(F32), (tile, lists.shape[2]))
        table[...] = spread.T.astype(jnp.int32)


def upper_blocks(krylov):
    count = krylov // 8
    return [(i, j) for i in range(count) for j in range(i, count)]


def share_blocks(start, turn, local_ref, table_ref):
    krylov, tile = local_ref.shape
    lane = lax.broadcasted_iota(jnp.int32, (8, tile), 1)
    pairs = upper_blocks(krylov)
    for c in range(table_ref.shape[1]):
        value = jnp.zeros((8, tile), F32)
        for k, (i, j) in enumerate(pairs[2 * c : 2 * c + 2]):
            target = start + 8 * k
            moved = pltpu.roll(local_ref[8 * i : 8 * i + 8, :], (target - 8 * j) % tile, 1)
            value = jnp.where((lane >= target) & (lane < target + 8), moved, value)
        high = value.astype(BF16).astype(F32)
        both = high + pltpu.roll(value - high, 16, 1)
        table_ref[0, c] = both
        table_ref[1, c] = pltpu.roll(both, turn, 1)


def placed(piece, code, place):
    onehot = jnp.where(place == code, 1.0, 0.0).astype(BF16)
    return jnp.dot(onehot[:, : piece.shape[0]], piece, preferred_element_type=F32)


def tile_kernel(sizes, groups, first, cols_ref, rows_ref, gathered_ref, tiles_ref, *refs):
    refs, turned = refs[:-1], refs[-1]
    used = []
    region, cap, vectors = sizes
    tile = tiles_ref.shape[2]
    span = (cap + 1) * vectors
    position = lax.axis_index("col")
    if first:
        local_ref, out_refs, table = refs[0], refs[1:-1], refs[-1]
        share_blocks(cap * vectors, span, local_ref, table)
    else:
        table, out_refs = refs[0], refs[1:]
    lane = lax.broadcasted_iota(jnp.int32, (8, tile), 1)
    sublane = lax.broadcasted_iota(jnp.int32, (8, tile), 0)

    def column(t):
        c = cols_ref[pl.ds(t, 1), :1][0, 0]
        r = lax.div(c, region)
        x = gathered_ref[r, c - r * region]
        return [x[m * vectors : (m + 1) * vectors] for m in range(3)]

    def weights(m, t):
        return tiles_ref[m, pl.ds(t, 2)].reshape(2 * tile, tile)

    def through(lhs, rhs):
        slot = len(used)
        used.append(slot)
        turned[slot] = rhs.T
        return jnp.dot(lhs, turned[slot], preferred_element_type=F32)

    def side(a, b):
        return jnp.concatenate([a, b], axis=1)

    def block(core, distance, out_ref, place):
        target = (position ^ (2 * distance)) ^ core
        index = lax.rem(lane + core * (tile - span), tile)
        slot = index // vectors
        inner = index - slot * vectors
        base = target * cap

        def store(p, out):
            pair = jnp.concatenate([out[:vectors, :tile], out[vectors:, tile:]], axis=0)
            out_ref[place, 2 * p * vectors : (2 * p + 2) * vectors, :] = pair.astype(BF16)

        pairs = []
        for p in range(cap // 2):
            t = base + 2 * p
            x0, x1 = column(t), column(t + 1)
            lhs = jnp.concatenate([side(x0[0], x0[1]), side(x1[0], x1[1])], axis=0)
            rhs = side(weights(0, t), weights(1, t))
            third = jnp.concatenate([x0[2], x1[2]], axis=0)
            out = through(lhs, rhs)
            pairs.append((p, out, third, weights(2, t)))
        while len(pairs) > 1:
            (p, out_p, x_p, w_p), (q, out_q, x_q, w_q) = pairs[:2]
            pairs = pairs[2:]
            zero = jnp.zeros_like(x_p)
            lhs = jnp.concatenate([side(x_p, zero), side(zero, x_q)], axis=0)
            both = contract_lanes(lhs, side(w_p, w_q))
            store(p, out_p + both[: 2 * vectors])
            store(q, out_q + both[2 * vectors :])
        for p, out_p, x_p, w_p in pairs:
            store(p, out_p + contract_lanes(x_p, w_p))
        code = jnp.full((8, tile), -1, jnp.int32)
        for s in range(cap):
            code = jnp.where(
                slot == s, (rows_ref[pl.ds(base + s, 1), :] - target * region) * vectors + inner, code
            )
        coded = (sublane == 7) & (slot < cap)
        last = jnp.where(coded, code.astype(F32), table[core, target])
        out_ref[place, cap * vectors : (cap + 1) * vectors, :] = last.astype(BF16)

    for group, out_ref in zip(groups, out_refs):
        for place, (core, distance) in enumerate(group):
            block(core, distance, out_ref, place)


def own_kernel(sizes, own_ref, partner_ref, total_ref, small_ref):
    _, cap, vectors = sizes
    tile = total_ref.shape[1]
    span = (cap + 1) * vectors
    place = lax.broadcasted_iota(jnp.int32, total_ref.shape, 0).astype(F32)
    total = jnp.zeros(total_ref.shape, F32)
    small = jnp.zeros(small_ref.shape, F32)
    row_lane = lax.broadcasted_iota(jnp.int32, (1, tile), 1)
    for piece, shift in ((own_ref[0], 0), (partner_ref[0], tile - span)):
        last = piece[cap * vectors :].astype(F32)
        last = pltpu.roll(last, shift, 1) if shift else last
        small += last
        code = jnp.where(row_lane < cap * vectors, last[7:8, :], -1.0)
        total += placed(piece, code, place)
    total_ref[...] = total
    small_ref[...] = small


def merge_kernel(sizes, basis_ref, total_ref, small_ref, *refs):
    region, krylov, cap, vectors = sizes
    blocks, (applied_ref, packet_ref) = refs[:-2], refs[-2:]
    tile = applied_ref.shape[1] // region
    total = total_ref[...]
    small = small_ref[...]
    turned = jnp.zeros_like(small)
    place = lax.broadcasted_iota(jnp.int32, (region * vectors, 2 * tile), 0).astype(F32)
    span = (cap + 1) * vectors
    row_lane = lax.broadcasted_iota(jnp.int32, (1, tile), 1)
    for ref in blocks:
        piece = ref[...]
        near = piece[cap * vectors : span].astype(F32)
        far = piece[span + cap * vectors :].astype(F32)
        small += near
        turned += far
        near_code = jnp.where(row_lane < cap * vectors, near[7:8, :], -1.0)
        far_code = jnp.where(lax.rem(row_lane + tile - span, tile) < cap * vectors, far[7:8, :], -1.0)
        code = jnp.where(row_lane < span, near_code, far_code)
        total += placed(piece, jnp.concatenate([code, far_code], axis=1), place)
    for t in range(region):
        applied_ref[:, t * tile : (t + 1) * tile] = total[t * vectors : (t + 1) * vectors]
    applied = applied_ref[...]
    high, middle, _ = split3(applied)
    lhs = jnp.concatenate([high, middle], axis=0).astype(BF16)
    inner = contract_lanes(lhs, basis_ref[...])
    raw = inner[:vectors] + inner[vectors:]
    cross = contract_lanes(lhs, lhs)
    energy = (cross[:vectors, :vectors] + cross[vectors:, vectors:]) + (
        cross[:vectors, vectors:] + cross[vectors:, :vectors]
    )
    small += pltpu.roll(turned, tile - span, 1)
    small += pltpu.roll(small, tile - 16, 1)
    lane = lax.broadcasted_iota(jnp.int32, (vectors, tile), 1)
    used = krylov + vectors
    packet = jnp.concatenate([raw, energy, jnp.zeros((vectors, tile - used), F32)], axis=1)
    moved = pltpu.roll(small, (HALF - 16 - cap * vectors) % tile, 1)
    packet = jnp.where((lane >= HALF - 16) & (lane < HALF), moved, packet)
    folded = jnp.where(
        lane[: vectors // 2] < HALF,
        packet[: vectors // 2],
        pltpu.roll(packet, HALF, 1)[vectors // 2 :],
    )
    packet_ref[...] = jnp.broadcast_to(folded[None], packet_ref.shape)


def tree_sum(values):
    while len(values) > 1:
        values = [sum(values[i : i + 2]) for i in range(0, len(values), 2)]
    return values[0]


def finish_kernel(
    sizes, packets_ref, applied_ref, basis_ref, new_ref, coefficients_ref, factor_ref
):
    krylov, vectors, col_count, entries = sizes
    inverse_root = 1.0 / math.sqrt(entries)
    devices, _, tile = packets_ref.shape
    row_count = devices // col_count
    shares = [
        tree_sum([packets_ref[r * col_count + c] for r in range(row_count)])
        for c in range(col_count)
    ]
    folded = tree_sum(shares)
    total = jnp.concatenate([folded, pltpu.roll(folded, HALF, 1)], axis=0)
    lane = lax.broadcasted_iota(jnp.int32, (vectors, tile), 1)
    zero = jnp.zeros((vectors, tile), F32)
    upper = [zero] * (krylov // 8)
    strict = [zero] * (krylov // 8)
    for n, (i, j) in enumerate(upper_blocks(krylov)):
        part = shares[n // 2] * (1.0 / entries)
        part = jnp.concatenate([part, pltpu.roll(part, HALF, 1)], axis=0)
        moved = pltpu.roll(part, (8 * j - (HALF - 16) - 8 * (n % 2)) % tile, 1)
        here = (lane >= 8 * j) & (lane < 8 * j + 8)
        upper[i] = jnp.where(here, moved, upper[i])
        if i < j:
            strict[i] = jnp.where(here, moved, strict[i])
    upper = jnp.concatenate(upper, axis=0)[:, :krylov]
    strict = jnp.concatenate(strict, axis=0)[:, :krylov]
    first = total[:, :krylov] * inverse_root
    energy = total[:, krylov : krylov + vectors]
    upper_high, strict_high = upper.astype(BF16), strict.astype(BF16)
    upper_low = (upper - upper_high.astype(F32)).astype(BF16)
    strict_low = (strict - strict_high.astype(F32)).astype(BF16)

    def halves(value):
        high = value.astype(BF16).astype(F32)
        return high.astype(BF16), jnp.concatenate([high, value - high], axis=0).astype(BF16)

    def times_correlation(value):
        high, both = halves(value)
        main = jnp.dot(both, upper_high, preferred_element_type=F32)
        main += contract_lanes(both, strict_high)
        rest = jnp.dot(high, upper_low, preferred_element_type=F32)
        rest += contract_lanes(high, strict_low)
        return main[:vectors] + (main[vectors:] + rest)

    coefficients = first + (first - times_correlation(first))
    coefficients_ref[...] = coefficients
    _, parts = halves(coefficients * inverse_root)
    wide = jnp.dot(parts, basis_ref[...], preferred_element_type=F32)
    cleaned = applied_ref[...] - (wide[:vectors] + wide[vectors:])
    coef_high, coef_both = halves(coefficients)
    high, both = halves(times_correlation(coefficients) - 2.0 * first)
    main = contract_lanes(both, coef_high)
    rest = contract_lanes(high, coef_both[vectors:])
    gram = (energy + main[:vectors] + (main[vectors:] + rest)) * (1.0 / entries)
    columns = [jnp.broadcast_to(gram[:, j : j + 1], (vectors, tile)) for j in range(vectors)]
    sublane = lax.broadcasted_iota(jnp.int32, (vectors, tile), 0)
    lane = lax.broadcasted_iota(jnp.int32, (vectors, tile), 1)
    factor = jnp.zeros((vectors, tile), F32)
    length = cleaned.shape[1]
    for j in range(vectors):
        inverse = lax.rsqrt(columns[j][j : j + 1, :])
        column = jnp.where(sublane >= j, columns[j] * inverse, 0.0)
        factor = jnp.where(lane == j, column, factor)
        for k in range(j + 1, vectors):
            columns[k] = columns[k] - column * column[k : k + 1, :]
        below = jnp.where(sublane > j, column, 0.0)
        pieces = []
        for t in range(length // tile):
            piece = cleaned[:, t * tile : (t + 1) * tile]
            row = piece[j : j + 1, :] * inverse
            pieces.append(jnp.where(sublane == j, row, piece - below * row))
        cleaned = jnp.concatenate(pieces, axis=1)
    factor_ref[...] = factor[:, :vectors]
    new_ref[...] = cleaned


def shards(basis, expand, tiles, tile_rows, tile_cols):
    row_count = lax.axis_size("row")
    col_count = lax.axis_size("col")
    krylov, length = basis.shape
    tile = tiles.shape[2]
    vectors = expand.shape[1]
    rows = expand.shape[0] * vectors
    region = length // tile
    devices = row_count * col_count
    entries = length * devices
    cap = tiles.shape[1] // col_count
    span = (cap + 1) * vectors
    assert krylov % 8 == 0 and krylov + vectors <= HALF - 16 and tile == 2 * HALF
    assert len(upper_blocks(krylov)) <= 2 * col_count and region * vectors <= 256
    assert vectors == 8 and cap % 2 == 0 and cap * vectors + 32 <= tile
    vmem = pl.BlockSpec(memory_space=pltpu.VMEM)
    hbm = pl.BlockSpec(memory_space=pltpu.HBM)

    count = tile_cols.shape[0]
    index_table = jax.ShapeDtypeStruct((count, tile), jnp.int32)
    series, local, wide_cols, wide_rows = pl.pallas_call(
        functools.partial(series_kernel, region, tile),
        out_shape=(
            jax.ShapeDtypeStruct((region, rows, tile), BF16),
            jax.ShapeDtypeStruct((krylov, tile), F32),
            index_table,
            index_table,
        ),
        in_specs=[hbm] * 4,
        out_specs=(vmem,) * 4,
        scratch_shapes=[
            pltpu.VMEM(basis.shape, BF16),
            pltpu.VMEM((rows, krylov), F32),
            pltpu.VMEM((2, 1, count), jnp.int32),
            pltpu.SemaphoreType.DMA((krylov // 8 + 3,)),
        ],
        cost_estimate=pl.CostEstimate(flops=10**10, bytes_accessed=10**7, transcendentals=0),
        compiler_params=pltpu.CompilerParams(vmem_limit_bytes=4 << 20),
        name="series",
    )(
        *(
            pltpu.with_memory_space_constraint(value, pltpu.HBM)
            for value in (
                basis,
                expand.reshape(rows, krylov),
                tile_cols.reshape(1, count),
                tile_rows.reshape(1, count),
            )
        )
    )
    gathered = lax.all_gather(series, "row", axis=0)
    half = col_count // 2
    sizes = (region, cap, vectors)

    def products(groups, given, first=False):
        shapes = [((len(group), span, tile), BF16) for group in groups]
        shapes += [((2, col_count, 8, tile), F32)] * first
        weights = 9 * sum(map(len, groups))
        return pl.pallas_call(
            functools.partial(tile_kernel, sizes, groups, first),
            out_shape=tuple(jax.ShapeDtypeStruct(*shape) for shape in shapes),
            in_specs=[vmem] * 5,
            out_specs=(vmem,) * len(shapes),
            scratch_shapes=[pltpu.VMEM((weights, 2 * tile, 2 * tile), BF16)],
            cost_estimate=pl.CostEstimate(
                flops=5 * 10**9, bytes_accessed=10**7, transcendentals=0
            ),
            compiler_params=pltpu.CompilerParams(vmem_limit_bytes=16 << 20),
            name="products",
        )(wide_cols, wide_rows, gathered, tiles, given)

    apart = tuple(range(half - 1, 0, -1))
    swap = [(i, i ^ 1) for i in range(col_count)]
    other, table = products((tuple((1, d) for d in apart),), local, True)
    partner = lax.ppermute(other, "col", swap)
    (mine,) = products((tuple((0, d) for d in apart),), table)
    other_here, own = products((((1, 0),), ((0, 0),)), table)
    partner_here = lax.ppermute(other_here, "col", swap)
    blocks = list(
        pl.pallas_call(
            functools.partial(own_kernel, sizes),
            out_shape=(
                jax.ShapeDtypeStruct((region * vectors, tile), F32),
                jax.ShapeDtypeStruct((vectors, tile), F32),
            ),
            in_specs=[vmem] * 2,
            out_specs=(vmem,) * 2,
            cost_estimate=pl.CostEstimate(flops=5 * 10**8, bytes_accessed=10**6, transcendentals=0),
            compiler_params=pltpu.CompilerParams(vmem_limit_bytes=8 << 20),
            name="own",
        )(own, partner_here)
    )
    for place, distance in enumerate(apart):
        moves = [(i, i ^ (2 * distance)) for i in range(col_count)]
        pair = jnp.concatenate([mine[place], partner[place]], axis=0)
        blocks.append(lax.ppermute(pair, "col", moves))
    applied, packet = pl.pallas_call(
        functools.partial(merge_kernel, (region, krylov, cap, vectors)),
        out_shape=(
            jax.ShapeDtypeStruct((vectors, length), F32),
            jax.ShapeDtypeStruct((devices, vectors // 2, tile), F32),
        ),
        in_specs=[vmem] * (1 + len(blocks)),
        out_specs=(vmem, vmem),
        compiler_params=pltpu.CompilerParams(vmem_limit_bytes=8 << 20),
        name="merge",
    )(basis, *blocks)
    packets = lax.all_to_all(packet, ("row", "col"), 0, 0, tiled=True)
    return pl.pallas_call(
        functools.partial(finish_kernel, (krylov, vectors, col_count, entries)),
        out_shape=(
            jax.ShapeDtypeStruct((vectors, length), F32),
            jax.ShapeDtypeStruct((vectors, krylov), F32),
            jax.ShapeDtypeStruct((vectors, vectors), F32),
        ),
        in_specs=[vmem] * 3,
        out_specs=(vmem,) * 3,
        compiler_params=pltpu.CompilerParams(vmem_limit_bytes=4 << 20),
        name="finish",
    )(packets, applied, basis)


def solution(mesh):
    return jax.shard_map(
        shards,
        mesh=mesh,
        in_specs=(
            P(None, ("row", "col")),
            P(),
            P(None, ("row", "col"), None, None),
            P(("row", "col")),
            P(("row", "col")),
        ),
        out_specs=(P(None, ("row", "col")), P(), P()),
        check_vma=False,
    )
```
